128 devices in a mesh: rows: 16 (over y, x), cols: 8 (over z, core).
Axes of the slice: x: 4, y: 4, z: 4, core: 2. Of those that a mesh axis runs over, the one named last changes fastest.
Arguments:
- fmap1: bfloat16 [2, 512, 512, 256], P(None, 'rows', 'cols'), may hold values from -6 to 6
- fmap2: bfloat16 [2, 512, 512, 256], P(None, 'rows', 'cols'), may hold values from -6 to 6
- target_owner: int32 [2, 8192, 1], P(None, ('rows', 'cols')), may hold values from 0 to 127; in each aligned block of 64 rows (0 to 63, 64 to 127, ..., all dimensions but the last counted through in order) at most 2 rows name the same one
- target_tile: int32 [2, 8192], P(None, ('rows', 'cols')), may hold values from 0 to 31
Outputs:
- corr: float32 [2, 81, 524288], P(None, None, ('rows', 'cols'))
The draws below stay inside these ranges and needn't reach their ends.
Inputs may be any that keep to these rules, and one draw needn't show every extreme that they name: `target_owner`: at each level, the 64 query blocks of one region (aligned blocks of rows) name any one owner at most 2 times, a bound that some block reaches. `target_tile`: tile of the owner's region in the query block's frame, numbered row-major; level l uses it modulo that level's tile count.
All inputs are finite; a program needn't handle non-finite values.
Results may differ from the reference program's by a relative error of at most 0.0013.
Values may be sent and summed in bfloat16 or wider, within the bound.
No kernel may reach another device: no remote copies, remote signals or barrier semaphores. Data moves between devices by JAX's collectives and lax.ppermute only.
A program may use at most 128 MiB of HBM per device.

```python
import math
import jax
import jax.numpy as jnp
import numpy as np
from jax import lax

C = 256
RADIUS = 4
LEVELS = 2
BATCH = 2
QH = 32
QW = 64
H0 = 512
W0 = 512
TILES = 32
QB_DEV = 64
CAP = 2
QBLK = 8192
N_ROWS = 16
N_COLS = 8


def with_ends(entries, stream_key, low, high):
    place = [jax.random.randint(jax.random.fold_in(stream_key, axis), (), 0, length) for axis, length in enumerate(entries.shape)]
    longest = entries.shape.index(max(entries.shape))
    neighbour = place[:longest] + [(place[longest] + 1) % entries.shape[longest]] + place[longest + 1:]
    return entries.at[tuple(place)].set(low).at[tuple(neighbour)].set(high)


def block_scale(key, extent, shards, low, largest):
    loudness, own = 1.0, jax.random.fold_in(key, 6)
    for axis_at, parts in shards:
        steps = jnp.exp(jax.random.uniform(jax.random.fold_in(own, axis_at), (parts,), jnp.float32, low / len(shards), largest / len(shards)))
        loudness = loudness * jnp.repeat(steps, extent[axis_at] // parts).reshape([-1 if axis == axis_at else 1 for axis in range(len(extent))])
    return loudness


def routed_block(own_key, own, number, rows, amount, top, reach, skew):
    order = jax.random.permutation(own_key, amount)
    packed, common = portions_of(amount, rows * top, reach, skew, True), portions_of(amount, rows * top, reach, skew, False)
    places = jnp.arange(amount)

    def named(tallies, offset_by):
        used = int((tallies > 0).sum())
        fixed = max(1, used // 4)
        passed = fixed + (places - fixed + offset_by * (used - fixed)) % max(1, amount - fixed)
        return jnp.zeros((amount,), jnp.int32).at[order[jnp.where(places < fixed, places, passed)]].set(jnp.asarray(tallies, jnp.int32))

    tallies = jnp.where(number % 4 == 0, named(packed, number // 4), named(common, number - number // 4 - 1))
    mixed = jax.random.permutation(jax.random.fold_in(own, 3), amount)
    source_of, receiver = mixed[0:amount // 2 * 2:2], mixed[1:amount // 2 * 2:2]
    margin = jnp.minimum(tallies[source_of] - 1, reach - tallies[receiver]) // 2
    margin = jnp.where((source_of == order[0]) | (receiver == order[0]) | (tallies[receiver] == 0), 0, jnp.maximum(margin, 0))
    passed = jax.random.randint(jax.random.fold_in(own, 4), (amount // 2,), 0, 1 << 20) % (margin + 1)
    tallies = tallies.at[source_of].add(-passed).at[receiver].add(passed)
    members = jnp.searchsorted(jnp.cumsum(tallies), jnp.arange(rows * top), side="right").astype(jnp.int32)
    table = members.reshape(top, rows).T
    table = table[jax.random.permutation(jax.random.fold_in(own, 1), rows)]
    offset_by = jax.random.randint(jax.random.fold_in(own, 2), (rows, 1), 0, top)
    return jnp.take_along_axis(table, (jnp.arange(top)[None, :] + offset_by) % top, axis=1)


def portions_of(number_of, total, reach, skew, full):
    weights = [(1 << 20) // math.isqrt(standing ** skew) + 1 for standing in range(1, number_of + 1)]
    largest = reach if full else min(reach, max(-(-total // number_of), total * weights[0] // sum(weights)))
    least = 1 if total - largest >= number_of - 1 else 0
    holding, rest = [largest] + [least] * (number_of - 1), total - largest - least * (number_of - 1)
    while rest > 0:
        candidates = [i for i in range(1, number_of) if holding[i] < largest] or [i for i in range(1, number_of) if holding[i] < reach]
        whole, remaining = sum([weights[i] for i in candidates]), rest
        for i in candidates:
            extra = min(reach - holding[i], max(1, remaining * weights[i] // whole), rest)
            holding[i] = holding[i] + extra
            rest = rest - extra
    return np.array(holding)


def noise(key, shape, spread, most, shards=(), kind=jnp.bfloat16):
    array = jax.random.normal(key, shape, jnp.float32) * spread
    if len(shards) > 0:
        array = block_scale(key, shape, shards, -0.22, 0.18) * array
    return jnp.clip(array, min=-most, max=most).astype(kind)


def setup_inputs(seed: int = 0) -> dict:
    key_list = jax.random.split(jax.random.key(seed), 5)
    fmap1 = noise(key_list[0], (BATCH, H0, W0, C), 1.0, 6.0, ((1, 16), (2, 8)))
    fmap2 = noise(key_list[1], (BATCH, H0, W0, C), 1.0, 6.0, ((1, 16), (2, 8)))
    target_owner_keys = jax.random.split(jax.random.fold_in(key_list[2], 1), LEVELS * QBLK // QB_DEV)
    target_owner_turns = jax.random.permutation(jax.random.fold_in(key_list[2], 3), LEVELS * QBLK // QB_DEV)
    target_owner = jax.vmap(lambda own, number: routed_block(jax.random.fold_in(key_list[2], 2), own, number, QB_DEV, N_ROWS * N_COLS, 1, CAP, 2))(target_owner_keys, target_owner_turns).reshape((LEVELS, QBLK, 1))
    target_tile = with_ends(jax.random.randint(key_list[3], (LEVELS, QBLK), 0, TILES), jax.random.fold_in(key_list[3], 1), 0, TILES - 1).astype(jnp.int32)
    return dict(fmap1=fmap1, fmap2=fmap2, target_owner=target_owner, target_tile=target_tile)


def window_index():
    tile_side = 2 * RADIUS
    span_side = 4 * RADIUS
    window_side = 2 * RADIUS + 1
    query_ids = jnp.arange(tile_side * tile_side, dtype=jnp.int32)
    offset_ids = jnp.arange(window_side * window_side, dtype=jnp.int32)
    row_part = query_ids[:, None] // tile_side + offset_ids[None, :] // window_side
    col_part = query_ids[:, None] % tile_side + offset_ids[None, :] % window_side
    return row_part * span_side + col_part


def pool_level(level_map):
    frame_count, rows_in, cols_in, channels = level_map.shape
    pooled = level_map.astype(jnp.float32).reshape(frame_count, rows_in // 2, 2, cols_in // 2, 2, channels)
    return jnp.mean(pooled, axis=(2, 4)).astype(jnp.bfloat16)


def reference(fmap1, fmap2, target_owner, target_tile):
    tile_side = 2 * RADIUS
    span_side = 4 * RADIUS
    window_side = 2 * RADIUS + 1
    device_count = N_ROWS * N_COLS
    levels = [fmap2]
    for level in range(1, LEVELS):
        levels.append(pool_level(levels[-1]))
    padded = [jnp.pad(level_map, ((0, 0), (RADIUS, RADIUS), (RADIUS, RADIUS), (0, 0))) for level_map in levels]
    window_ids = window_index()
    tiles_across = QW // tile_side
    per_frame = (QH // tile_side) * tiles_across
    block_ids = jnp.arange(QB_DEV, dtype=jnp.int32)
    frame_ids = block_ids // per_frame
    block_rows = (block_ids % per_frame) // tiles_across * tile_side
    block_cols = block_ids % tiles_across * tile_side
    owner_table = target_owner[:, :, 0].reshape(LEVELS, device_count, QB_DEV)
    tile_table = target_tile.reshape(LEVELS, device_count, QB_DEV)
    gather_ids = jnp.broadcast_to(window_ids[None], (QB_DEV,) + window_ids.shape)

    def one_device(device):
        first_row = device // N_COLS * QH + block_rows
        first_col = device % N_COLS * QW + block_cols

        def query_block(frame_id, row_at, col_at):
            return lax.dynamic_slice(fmap1, (frame_id, row_at, col_at, 0 * frame_id), (1, tile_side, tile_side, C)).reshape(tile_side * tile_side, C)

        queries = jax.vmap(query_block)(frame_ids, first_row, first_col).astype(jnp.float32)
        results = []
        for level in range(LEVELS):
            level_rows = QH >> level
            level_cols = QW >> level
            level_across = level_cols // tile_side
            tile_count = (level_rows // tile_side) * level_across
            owner_ids = owner_table[level, device]
            tile_ids = tile_table[level, device] % tile_count
            target_rows = owner_ids // N_COLS * level_rows + tile_ids // level_across * tile_side
            target_cols = owner_ids % N_COLS * level_cols + tile_ids % level_across * tile_side

            def target_block(frame_id, row_at, col_at, source=padded[level]):
                return lax.dynamic_slice(source, (frame_id, row_at, col_at, 0 * frame_id), (1, span_side, span_side, C)).reshape(span_side * span_side, C)

            targets = jax.vmap(target_block)(frame_ids, target_rows, target_cols).astype(jnp.float32)
            scores = jnp.einsum("bqc,bpc->bqp", queries, targets, precision=lax.Precision.HIGHEST) * C ** -0.5
            results.append(jnp.take_along_axis(scores, gather_ids, axis=2))
        return jnp.stack(results)

    stacked = lax.map(one_device, jnp.arange(device_count, dtype=jnp.int32))
    return stacked.transpose(1, 4, 0, 2, 3).reshape(LEVELS, window_side * window_side, device_count * QB_DEV * tile_side * tile_side)
```

```python
import jax
import jax.numpy as jnp
from jax import lax
from jax.experimental import pallas as pl
from jax.experimental.pallas import tpu as pltpu
from jax.sharding import PartitionSpec as P

RADIUS = 4
LEVELS = 2
SIDE = 2 * RADIUS
SPAN = 4 * RADIUS
WIN = 2 * RADIUS + 1
WINDOW = WIN * WIN
QUERIES = SIDE * SIDE
SLOTS = 2
LANES = SLOTS * QUERIES
REPLY_ROWS = -(-(WINDOW + 1) // 8) * 8
PEERS_A_STEP = 8
FULL = 32767.0
AXES = ("rows", "cols")


def halo(block, axis, dim, width):
    count = lax.axis_size(axis)
    forward = [(i, i + 1) for i in range(count - 1)]
    backward = [(target, source) for source, target in forward]
    low = lax.ppermute(
        lax.slice_in_dim(block, block.shape[dim] - width, None, axis=dim), axis, forward
    )
    high = lax.ppermute(lax.slice_in_dim(block, 0, width, axis=dim), axis, backward)
    return jnp.concatenate([low, block, high], axis=dim)


def pool_level(level_map):
    frame_count, rows_in, cols_in, channels = level_map.shape
    pooled = level_map.astype(jnp.float32).reshape(
        frame_count, rows_in // 2, 2, cols_in // 2, 2, channels
    )
    return jnp.mean(pooled, axis=(2, 4)).astype(jnp.bfloat16)


def window_strips(padded):
    frames, rows, cols, channels = padded.shape
    across = (cols - SIDE) // SIDE
    strips = [
        lax.slice_in_dim(padded, t * SIDE, t * SIDE + SPAN, axis=2) for t in range(across)
    ]
    return jnp.stack(strips).reshape(across * frames * rows, SPAN, channels)


def build_body(peers, blocks, tiles_of, per_frame, across, band_rows):
    def kernel(owner, tile, fmap, send0, send1, labels, slots, count, sems):
        sends = (send0, send1)

        def clear(i, carry):
            count[i] = 0
            return carry

        lax.fori_loop(0, LEVELS * peers, clear, 0, unroll=8)

        def blank(i, carry):
            labels[i] = -1
            return carry

        lax.fori_loop(0, LEVELS * SLOTS * peers, blank, 0, unroll=8)

        def source(k):
            frame = k // per_frame
            rest = k % per_frame
            row = frame * band_rows + rest // across * SIDE
            return fmap.at[pl.ds(row, SIDE), rest % across]

        def place(k, carry):
            for level in range(LEVELS):
                own = owner[level * blocks + k]
                seen = count[level * peers + own]
                count[level * peers + own] = seen + 1
                label = k // per_frame * tiles_of[level] + lax.rem(
                    tile[level * blocks + k], tiles_of[level]
                )
                labels[(level * peers + own) * SLOTS + seen] = label
                slot = own * SLOTS + seen
                slots[level * blocks + k] = slot
                pltpu.make_async_copy(
                    source(k), sends[level].at[slot], sems.at[level * blocks + k]
                ).start()
            return carry

        lax.fori_loop(0, blocks, place, 0)

        def finish(k, carry):
            for level in range(LEVELS):
                pltpu.make_async_copy(
                    source(k),
                    sends[level].at[slots[level * blocks + k]],
                    sems.at[level * blocks + k],
                ).wait()
            return carry

        lax.fori_loop(0, blocks, finish, 0)

    return kernel


def serve_body(rows, across, tiles, frames):
    def kernel(labels, queries, strips, reply, flat):
        step = pl.program_id(0)
        lane = lax.broadcasted_iota(jnp.int32, (1, LANES), 1)
        first = lane < QUERIES
        i_part = lane % QUERIES // SIDE
        j_part = lane % SIDE
        row_id = lax.broadcasted_iota(jnp.int32, (REPLY_ROWS, LANES), 0)
        flat[...] = jnp.zeros_like(flat)

        def start_of(label):
            label = jnp.maximum(label, 0)
            frame = label // tiles
            tile = label % tiles
            return (tile % across * frames + frame) * rows + tile // across * SIDE

        for peer in range(PEERS_A_STEP):
            at = (step * PEERS_A_STEP + peer) * SLOTS
            query = queries[peer]
            tables = []
            for slot in range(SLOTS):
                cells = strips[pl.ds(start_of(labels[at + slot]), SPAN)]
                tables.append(
                    lax.dot_general(
                        cells.reshape(SPAN * SPAN, -1),
                        query,
                        (((1,), (1,)), ((), ())),
                        preferred_element_type=jnp.float32,
                    )
                )
            table = jnp.where(first, tables[0], tables[1])
            table = table.reshape(SPAN, SPAN, LANES)
            for bit in (4, 2, 1):
                left = table.shape[0] - bit
                table = jnp.where(i_part & bit != 0, table[bit:], table[:left])
            table = table.reshape(WIN * SPAN, LANES)
            for bit in (4, 2, 1):
                table = jnp.where(
                    j_part & bit != 0, pltpu.roll(table, WIN * SPAN - bit, 0), table
                )
            for a in range(WIN):
                flat[peer, a * WIN : (a + 1) * WIN, :] = table[a * SPAN : a * SPAN + WIN]
            values = flat[peer]
            top = jnp.max(jnp.abs(values), axis=0, keepdims=True)
            power = jnp.ceil(jnp.log2(jnp.maximum(top, 1e-30)))
            coded = jnp.round(values * (jnp.exp2(-power) * FULL))
            coded = jnp.clip(coded, -FULL, FULL)
            coded = jnp.where(row_id == WINDOW, power, coded)
            reply[peer] = coded.astype(jnp.int32).astype(jnp.int16)

    return kernel


def finish_body(blocks, groups, scale):
    def kernel(slots, reply0, reply1, out):
        step = pl.program_id(0)
        low = lax.broadcasted_iota(jnp.int32, (1, LANES), 1) < QUERIES
        for level, reply in enumerate((reply0, reply1)):
            for group in range(groups):
                k = level * blocks + (step * groups + group) * 2
                halves = []
                for side in range(2):
                    slot = slots[k + side]
                    block = reply[slot // SLOTS].astype(jnp.int32)
                    turned = pltpu.roll(block, QUERIES, 1)
                    halves.append(jnp.where(slot % SLOTS == side, block, turned))
                both = jnp.where(low, halves[0], halves[1]).astype(jnp.float32)
                factor = jnp.exp2(both[WINDOW : WINDOW + 1]) * (scale / FULL)
                out[level, :, group * LANES : (group + 1) * LANES] = both[:WINDOW] * factor

    return kernel


def body(fmap1, fmap2, target_owner, target_tile):
    frames, band_rows, band_cols, channels = fmap1.shape
    peers = lax.axis_size("rows") * lax.axis_size("cols")
    across = band_cols // SIDE
    per_frame = band_rows // SIDE * across
    blocks = frames * per_frame
    tiles_of = [((band_rows >> l) // SIDE) * ((band_cols >> l) // SIDE) for l in range(LEVELS)]

    smem = pl.BlockSpec(memory_space=pltpu.SMEM)
    hbm = pl.BlockSpec(memory_space=pl.ANY)
    send_shape = jax.ShapeDtypeStruct((peers * SLOTS, SIDE, SIDE, channels), jnp.bfloat16)
    send0, send1, labels, slots = pl.pallas_call(
        build_body(peers, blocks, tiles_of, per_frame, across, band_rows),
        in_specs=[smem, smem, hbm],
        out_specs=[hbm, hbm, smem, smem],
        out_shape=[
            send_shape,
            send_shape,
            jax.ShapeDtypeStruct((LEVELS * peers * SLOTS,), jnp.int32),
            jax.ShapeDtypeStruct((LEVELS * blocks,), jnp.int32),
        ],
        scratch_shapes=[
            pltpu.SMEM((LEVELS * peers,), jnp.int32),
            pltpu.SemaphoreType.DMA((LEVELS * blocks,)),
        ],
        name="build",
    )(
        target_owner.reshape(LEVELS * blocks),
        target_tile.reshape(LEVELS * blocks),
        fmap1.reshape(frames * band_rows, across, SIDE, channels),
    )

    def exchange(value):
        return lax.all_to_all(value, AXES, split_axis=0, concat_axis=0, tiled=True)

    arrived = [
        exchange(send.reshape(peers, LANES, channels)) for send in (send0, send1)
    ]
    labels = labels.reshape(LEVELS, peers, SLOTS).transpose(1, 0, 2)
    labels = exchange(labels.reshape(peers, 1, LEVELS * SLOTS))
    labels = labels.reshape(peers, LEVELS, SLOTS).transpose(1, 0, 2).reshape(LEVELS, peers * SLOTS)

    wide = halo(halo(fmap2, "rows", 1, SIDE), "cols", 2, SIDE)
    maps = [wide[:, RADIUS:-RADIUS, RADIUS:-RADIUS], pool_level(wide)]

    replies = []
    for level in range(LEVELS):
        level_rows = maps[level].shape[1]
        strips = window_strips(maps[level])
        served = pl.pallas_call(
            serve_body(level_rows, (band_cols >> level) // SIDE, tiles_of[level], frames),
            grid_spec=pltpu.PrefetchScalarGridSpec(
                num_scalar_prefetch=1,
                grid=(peers // PEERS_A_STEP,),
                in_specs=[
                    pl.BlockSpec((PEERS_A_STEP, LANES, channels), lambda s, _: (s, 0, 0)),
                    pl.BlockSpec(strips.shape, lambda s, _: (0, 0, 0)),
                ],
                out_specs=pl.BlockSpec((PEERS_A_STEP, REPLY_ROWS, LANES), lambda s, _: (s, 0, 0)),
                scratch_shapes=[pltpu.VMEM((PEERS_A_STEP, REPLY_ROWS, LANES), jnp.float32)],
            ),
            out_shape=jax.ShapeDtypeStruct((peers, REPLY_ROWS, LANES), jnp.int16),
            name=f"serve{level}",
        )(labels[level], arrived[level], strips)
        replies.append(exchange(served))

    groups = 4
    width = groups * LANES
    return pl.pallas_call(
        finish_body(blocks, groups, channels ** (-0.5)),
        grid_spec=pltpu.PrefetchScalarGridSpec(
            num_scalar_prefetch=1,
            grid=(blocks * QUERIES // width,),
            in_specs=[
                pl.BlockSpec((peers, REPLY_ROWS, LANES), lambda s, _: (0, 0, 0)),
                pl.BlockSpec((peers, REPLY_ROWS, LANES), lambda s, _: (0, 0, 0)),
            ],
            out_specs=pl.BlockSpec((LEVELS, WINDOW, width), lambda s, _: (0, 0, s)),
        ),
        out_shape=jax.ShapeDtypeStruct((LEVELS, WINDOW, blocks * QUERIES), jnp.float32),
        name="finish",
    )(slots, *replies)


def solution(mesh):
    in_specs = (
        P(None, "rows", "cols", None),
        P(None, "rows", "cols", None),
        P(None, AXES, None),
        P(None, AXES),
    )
    out_specs = P(None, None, AXES)
    return jax.shard_map(body, mesh=mesh, in_specs=in_specs, out_specs=out_specs, check_vma=False)
```

```python
import jax
import jax.numpy as jnp
from jax import lax
from jax.experimental import pallas as pl
from jax.experimental.pallas import tpu as pltpu
from jax.sharding import PartitionSpec as P


RADIUS = 4
LEVELS = 2
SIDE = 2 * RADIUS
SPAN = 4 * RADIUS
WIN = 2 * RADIUS + 1
WINDOW = WIN * WIN
QUERIES = SIDE * SIDE
SLOTS = 2
LANES = SLOTS * QUERIES
REPLY_ROWS = -(-LEVELS * (WINDOW + 1) // 8) * 8
PEERS_A_STEP = 4
LABELS = 64
FULL = 32767.0
AXES = ("rows", "cols")


def halo(block, axis, dim, width):
    count = lax.axis_size(axis)
    forward = [(i, i + 1) for i in range(count - 1)]
    backward = [(target, source) for source, target in forward]
    low = lax.ppermute(
        lax.slice_in_dim(block, block.shape[dim] - width, None, axis=dim), axis, forward
    )
    high = lax.ppermute(lax.slice_in_dim(block, 0, width, axis=dim), axis, backward)
    return jnp.concatenate([low, block, high], axis=dim)


def pool_level(level_map):
    frame_count, rows_in, cols_in, channels = level_map.shape
    pooled = level_map.astype(jnp.float32).reshape(
        frame_count, rows_in // 2, 2, cols_in // 2, 2, channels
    )
    return jnp.mean(pooled, axis=(2, 4)).astype(jnp.bfloat16)


def window_strips(padded):
    frames, rows, cols, channels = padded.shape
    across = (cols - SIDE) // SIDE
    strips = [
        lax.slice_in_dim(padded, t * SIDE, t * SIDE + SPAN, axis=2) for t in range(across)
    ]
    return jnp.stack(strips).reshape(across * frames * rows, SPAN, channels)


def build_body(peers, blocks, tiles_of, per_frame, across, band_rows):
    def kernel(owner, tile, fmap, send, codes, count, sems):
        def clear(i, carry):
            count[i] = 0
            return carry

        lax.fori_loop(0, LEVELS * peers, clear, 0, unroll=8)

        def source(k):
            frame = k // per_frame
            rest = k % per_frame
            row = frame * band_rows + rest // across * SIDE
            return fmap.at[pl.ds(row, SIDE), rest % across]

        def place(k, carry):
            for level in range(LEVELS):
                own = owner[level * blocks + k]
                seen = count[level * peers + own]
                count[level * peers + own] = seen + 1
                label = k // per_frame * tiles_of[level] + lax.rem(
                    tile[level * blocks + k], tiles_of[level]
                )
                slot = (own * LEVELS + level) * SLOTS + seen
                codes[level * blocks + k] = slot * LABELS + label
                pltpu.make_async_copy(
                    source(k), send.at[slot], sems.at[level * blocks + k]
                ).start()
            return carry

        lax.fori_loop(0, blocks, place, 0)

        def finish(k, carry):
            for level in range(LEVELS):
                slot = codes[level * blocks + k] // LABELS
                pltpu.make_async_copy(
                    source(k), send.at[slot], sems.at[level * blocks + k]
                ).wait()
            return carry

        lax.fori_loop(0, blocks, finish, 0)

    return kernel


def serve_body(rows_of, across_of, tiles_of, frames):
    def kernel(labels, queries, strips0, strips1, reply, flat):
        step = pl.program_id(0)
        lane = lax.broadcasted_iota(jnp.int32, (1, LANES), 1)
        first = lane < QUERIES
        i_part = lane % QUERIES // SIDE
        j_part = lane % SIDE
        row_id = lax.broadcasted_iota(jnp.int32, (REPLY_ROWS, LANES), 0)
        flat[...] = jnp.zeros_like(flat)

        def start_of(label, level):
            label = jnp.maximum(label, 0)
            frame = label // tiles_of[level]
            tile = label % tiles_of[level]
            column = tile % across_of[level]
            return (column * frames + frame) * rows_of[level] + tile // across_of[level] * SIDE

        def table_of(peer, level, strips):
            at = ((step * PEERS_A_STEP + peer) * LEVELS + level) * SLOTS
            query = queries[peer, level * LANES : (level + 1) * LANES]
            tables = []
            for slot in range(SLOTS):
                cells = strips[pl.ds(start_of(labels[at + slot], level), SPAN)]
                tables.append(
                    lax.dot_general(
                        cells.reshape(SPAN * SPAN, -1),
                        query,
                        (((1,), (1,)), ((), ())),
                        preferred_element_type=jnp.float32,
                    )
                )
            table = jnp.where(first, tables[0], tables[1])
            table = table.reshape(SPAN, SPAN, LANES)
            for bit in (4, 2, 1):
                left = table.shape[0] - bit
                table = jnp.where(i_part & bit != 0, table[bit:], table[:left])
            table = table.reshape(WIN * SPAN, LANES)
            for bit in (4, 2, 1):
                table = jnp.where(
                    j_part & bit != 0, pltpu.roll(table, WIN * SPAN - bit, 0), table
                )
            return table

        for peer in range(PEERS_A_STEP):
            powers = []
            for level, strips in enumerate((strips0, strips1)):
                table = table_of(peer, level, strips)
                base = level * WINDOW
                for a in range(WIN):
                    flat[peer, base + a * WIN : base + (a + 1) * WIN, :] = table[
                        a * SPAN : a * SPAN + WIN
                    ]
            values = flat[peer]
            size = jnp.abs(values)
            tops = [
                jnp.max(jnp.where(row_id < WINDOW, size, 0.0), axis=0, keepdims=True),
                jnp.max(jnp.where(row_id < WINDOW, 0.0, size), axis=0, keepdims=True),
            ]
            powers = [jnp.ceil(jnp.log2(jnp.maximum(top, 1e-30))) for top in tops]
            factors = [jnp.exp2(-power) * FULL for power in powers]
            coded = jnp.round(values * jnp.where(row_id < WINDOW, factors[0], factors[1]))
            coded = jnp.clip(coded, -FULL, FULL)
            for level in range(LEVELS):
                coded = jnp.where(row_id == LEVELS * WINDOW + level, powers[level], coded)
            reply[peer] = coded.astype(jnp.int32).astype(jnp.int16)

    return kernel


def finish_body(blocks, groups, scale):
    def kernel(slots, reply, out):
        step = pl.program_id(0)
        low = lax.broadcasted_iota(jnp.int32, (1, LANES), 1) < QUERIES
        for level in range(LEVELS):
            for group in range(groups):
                k = level * blocks + (step * groups + group) * 2
                halves = []
                for side in range(2):
                    slot = slots[k + side] // LABELS
                    block = reply[slot // (LEVELS * SLOTS)].astype(jnp.int32)
                    turned = pltpu.roll(block, QUERIES, 1)
                    halves.append(jnp.where(slot % SLOTS == side, block, turned))
                both = jnp.where(low, halves[0], halves[1]).astype(jnp.float32)
                power = both[LEVELS * WINDOW + level : LEVELS * WINDOW + level + 1]
                factor = jnp.exp2(power) * (scale / FULL)
                values = both[level * WINDOW : (level + 1) * WINDOW] * factor
                out[:, level, group * LANES : (group + 1) * LANES] = values

    return kernel


def steps(fmap1, fmap2, target_owner, target_tile):
    frames, band_rows, band_cols, channels = fmap1.shape
    peers = lax.axis_size("rows") * lax.axis_size("cols")
    across = band_cols // SIDE
    per_frame = band_rows // SIDE * across
    blocks = frames * per_frame
    across_of = [(band_cols >> l) // SIDE for l in range(LEVELS)]
    tiles_of = [((band_rows >> l) // SIDE) * across_of[l] for l in range(LEVELS)]
    per_peer = LEVELS * SLOTS

    smem = pl.BlockSpec(memory_space=pltpu.SMEM)
    hbm = pl.BlockSpec(memory_space=pl.ANY)
    send, codes = pl.pallas_call(
        build_body(peers, blocks, tiles_of, per_frame, across, band_rows),
        in_specs=[smem, smem, pl.BlockSpec(memory_space=pltpu.VMEM)],
        out_specs=[hbm, smem],
        out_shape=[
            jax.ShapeDtypeStruct((peers * per_peer, SIDE, SIDE, channels), jnp.bfloat16),
            jax.ShapeDtypeStruct((LEVELS * blocks,), jnp.int32),
        ],
        scratch_shapes=[
            pltpu.SMEM((LEVELS * peers,), jnp.int32),
            pltpu.SemaphoreType.DMA((LEVELS * blocks,)),
        ],
        name="build",
    )(
        target_owner.reshape(LEVELS * blocks),
        target_tile.reshape(LEVELS * blocks),
        fmap1.reshape(frames * band_rows, across, SIDE, channels),
    )

    def exchange(value):
        return lax.all_to_all(value, AXES, split_axis=0, concat_axis=0, tiled=True)

    arrived = exchange(send.reshape(peers, LEVELS * LANES, channels))

    every = lax.all_gather(codes, AXES)
    mine = lax.axis_index(AXES) * per_peer + jnp.arange(per_peer, dtype=jnp.int32)
    found = every[:, None, :] // LABELS == mine[None, :, None]
    labels = jnp.max(jnp.where(found, every[:, None, :] % LABELS, -1), axis=2).reshape(-1)

    tall = halo(fmap2, "rows", 1, SIDE)
    wide = halo(tall, "cols", 2, SIDE)
    maps = [wide[:, RADIUS:-RADIUS, RADIUS:-RADIUS], pool_level(wide)]
    strips = [window_strips(level_map) for level_map in maps]

    served = pl.pallas_call(
        serve_body([m.shape[1] for m in maps], across_of, tiles_of, frames),
        grid_spec=pltpu.PrefetchScalarGridSpec(
            num_scalar_prefetch=1,
            grid=(peers // PEERS_A_STEP,),
            in_specs=[
                pl.BlockSpec((PEERS_A_STEP, LEVELS * LANES, channels), lambda s, _: (s, 0, 0)),
                pl.BlockSpec(strips[0].shape, lambda s, _: (0, 0, 0)),
                pl.BlockSpec(strips[1].shape, lambda s, _: (0, 0, 0)),
            ],
            out_specs=pl.BlockSpec((PEERS_A_STEP, REPLY_ROWS, LANES), lambda s, _: (s, 0, 0)),
            scratch_shapes=[pltpu.VMEM((PEERS_A_STEP, REPLY_ROWS, LANES), jnp.float32)],
        ),
        out_shape=jax.ShapeDtypeStruct((peers, REPLY_ROWS, LANES), jnp.int16),
        name="serve",
    )(labels, arrived, *strips)
    reply = exchange(served)

    groups = 4
    width = groups * LANES
    out = pl.pallas_call(
        finish_body(blocks, groups, channels ** (-0.5)),
        grid_spec=pltpu.PrefetchScalarGridSpec(
            num_scalar_prefetch=1,
            grid=(blocks * QUERIES // width,),
            in_specs=[pl.BlockSpec((peers, REPLY_ROWS, LANES), lambda s, _: (0, 0, 0))],
            out_specs=pl.BlockSpec((WINDOW, LEVELS, width), lambda s, _: (0, 0, s)),
        ),
        out_shape=jax.ShapeDtypeStruct((WINDOW, LEVELS, blocks * QUERIES), jnp.float32),
        name="finish",
    )(codes, reply)
    return out.transpose(1, 0, 2)


def solution(mesh):
    in_specs = (
        P(None, "rows", "cols", None),
        P(None, "rows", "cols", None),
        P(None, AXES, None),
        P(None, AXES),
    )
    out_specs = P(None, None, AXES)
    return jax.shard_map(steps, mesh=mesh, in_specs=in_specs, out_specs=out_specs, check_vma=False)
```

```python
import jax
import jax.numpy as jnp
from jax import lax
from jax.experimental import pallas as pl
from jax.experimental.pallas import tpu as pltpu
from jax.sharding import PartitionSpec as P


RADIUS = 4
LEVELS = 2
SIDE = 2 * RADIUS
SPAN = 4 * RADIUS
WIN = 2 * RADIUS + 1
WINDOW = WIN * WIN
QUERIES = SIDE * SIDE
SLOTS = 2
LANES = SLOTS * QUERIES
REPLY_ROWS = -(-LEVELS * (WINDOW + 1) // 8) * 8
PEERS_A_STEP = 16
BENCHES = 4
FULL = 32767.0
AXES = ("rows", "cols")


def swapped(upward, downward, axis):
    count = lax.axis_size(axis)
    forward = [(i, i + 1) for i in range(count - 1)]
    backward = [(target, source) for source, target in forward]
    return lax.ppermute(upward, axis, forward), lax.ppermute(downward, axis, backward)


def neighbours(block, axis, dim, width):
    tail = lax.slice_in_dim(block, block.shape[dim] - width, None, axis=dim)
    return swapped(tail, lax.slice_in_dim(block, 0, width, axis=dim), axis)


def pool_level(level_map):
    frame_count, rows_in, cols_in, channels = level_map.shape
    pooled = level_map.astype(jnp.float32).reshape(
        frame_count, rows_in // 2, 2, cols_in // 2, 2, channels
    )
    return jnp.mean(pooled, axis=(2, 4)).astype(jnp.bfloat16)


def window_strips(padded):
    frames, rows, cols, channels = padded.shape
    across = (cols - SIDE) // SIDE
    strips = [
        lax.slice_in_dim(padded, t * SIDE, t * SIDE + SPAN, axis=2) for t in range(across)
    ]
    return jnp.stack(strips).reshape(across * frames * rows, SPAN, channels)


def build_body(peers, blocks, tiles_of, per_frame, across, band_rows):
    def kernel(owner, tile, fmap, send, codes, count, labels, notes, sems, note_sem):
        def clear(i, carry):
            count[i] = 0
            return carry

        lax.fori_loop(0, LEVELS * peers, clear, 0, unroll=8)

        def blank(i, carry):
            labels[i] = 0
            return carry

        lax.fori_loop(0, LEVELS * SLOTS * peers, blank, 0, unroll=8)

        def source(k):
            frame = k // per_frame
            rest = k % per_frame
            row = frame * band_rows + rest // across * SIDE
            return fmap.at[pl.ds(row, SIDE), rest % across]

        def copy(k, level, slot):
            own = slot // (LEVELS * SLOTS)
            place = slot % (LEVELS * SLOTS)
            return pltpu.make_async_copy(
                source(k), send.at[own, pl.ds(place * SIDE, SIDE)], sems.at[level * blocks + k]
            )

        def place(k, carry):
            for level in range(LEVELS):
                own = owner[level, 0, k]
                seen = count[level * peers + own]
                count[level * peers + own] = seen + 1
                slot = (own * LEVELS + level) * SLOTS + seen
                codes[level * blocks + k] = slot
                labels[slot] = k // per_frame * tiles_of[level] + lax.rem(
                    tile[level, k], tiles_of[level]
                )
                copy(k, level, slot).start()
            return carry

        lax.fori_loop(0, blocks, place, 0)

        lane = lax.broadcasted_iota(jnp.int32, notes.shape[1:], 1)

        def note(peer, carry):
            values = jnp.zeros(notes.shape[1:], jnp.int32)
            for slot in range(LEVELS * SLOTS):
                values = jnp.where(lane == slot, labels[peer * LEVELS * SLOTS + slot], values)
            notes[peer] = values.astype(jnp.float32).astype(jnp.bfloat16)
            return carry

        lax.fori_loop(0, peers, note, 0, unroll=4)
        noted = pltpu.make_async_copy(notes, send.at[:, LEVELS * SLOTS * SIDE], note_sem)
        noted.start()

        def finish(k, carry):
            for level in range(LEVELS):
                copy(k, level, codes[level * blocks + k]).wait()
            return carry

        lax.fori_loop(0, blocks, finish, 0)
        noted.wait()

    return kernel


def serve_body(rows_of, across_of, tiles_of, frames, peers):
    def kernel(notes, queries, strips0, strips1, reply, flat, lines, labels, sem):
        step = pl.program_id(0)
        lane = lax.broadcasted_iota(jnp.int32, (1, LANES), 1)
        first = lane < QUERIES
        i_part = lane % QUERIES // SIDE
        j_part = lane % SIDE
        row_id = lax.broadcasted_iota(jnp.int32, (REPLY_ROWS, LANES), 0)

        @pl.when(step == 0)
        def _():
            flat[...] = jnp.zeros_like(flat)

            def line(peer, carry):
                values = notes[peer].astype(jnp.float32).astype(jnp.int32)
                lines[pl.ds(peer, 1), :] = values[:1, : lines.shape[1]]
                return carry

            lax.fori_loop(0, peers, line, 0, unroll=8)
            taken = pltpu.make_async_copy(lines, labels, sem)
            taken.start()
            taken.wait()

        def start_of(label, level):
            frame = label // tiles_of[level]
            tile = label % tiles_of[level]
            column = tile % across_of[level]
            return (column * frames + frame) * rows_of[level] + tile // across_of[level] * SIDE

        def table_of(peer, level, strips):
            query = queries[peer, level * LANES : (level + 1) * LANES]
            tables = []
            for slot in range(SLOTS):
                label = labels[step * PEERS_A_STEP + peer, level * SLOTS + slot]
                cells = strips[pl.ds(start_of(label, level), SPAN)]
                tables.append(
                    lax.dot_general(
                        cells.reshape(SPAN * SPAN, -1),
                        query,
                        (((1,), (1,)), ((), ())),
                        preferred_element_type=jnp.float32,
                    )
                )
            table = jnp.where(first, tables[0], tables[1])
            table = table.reshape(SPAN, SPAN, LANES)
            for bit in (4, 2, 1):
                left = table.shape[0] - bit
                table = jnp.where(i_part & bit != 0, table[bit:], table[:left])
            table = table.reshape(WIN * SPAN, LANES)
            for bit in (4, 2, 1):
                table = jnp.where(
                    j_part & bit != 0, pltpu.roll(table, WIN * SPAN - bit, 0), table
                )
            return table

        def one(peer, bench):
            for level, strips in enumerate((strips0, strips1)):
                table = table_of(peer, level, strips)
                base = level * WINDOW
                for a in range(WIN):
                    flat[bench, base + a * WIN : base + (a + 1) * WIN, :] = table[
                        a * SPAN : a * SPAN + WIN
                    ]
            values = flat[bench]
            size = jnp.abs(values)
            tops = [
                jnp.max(jnp.where(row_id < WINDOW, size, 0.0), axis=0, keepdims=True),
                jnp.max(jnp.where(row_id < WINDOW, 0.0, size), axis=0, keepdims=True),
            ]
            powers = [jnp.ceil(jnp.log2(jnp.maximum(top, 1e-30))) for top in tops]
            factors = [jnp.exp2(-power) * FULL for power in powers]
            coded = jnp.round(values * jnp.where(row_id < WINDOW, factors[0], factors[1]))
            coded = jnp.clip(coded, -FULL, FULL)
            for level in range(LEVELS):
                coded = jnp.where(row_id == LEVELS * WINDOW + level, powers[level], coded)
            reply[peer] = coded.astype(jnp.int32).astype(jnp.int16)

        def turn(i, carry):
            for bench in range(BENCHES):
                one(i * BENCHES + bench, bench)
            return carry

        lax.fori_loop(0, PEERS_A_STEP // BENCHES, turn, 0)

    return kernel


def finish_body(blocks, groups, scale):
    def kernel(slots, reply, out):
        step = pl.program_id(0)
        low = lax.broadcasted_iota(jnp.int32, (1, LANES), 1) < QUERIES
        for level in range(LEVELS):
            for group in range(groups):
                k = level * blocks + (step * groups + group) * 2
                halves = []
                for side in range(2):
                    slot = slots[k + side]
                    block = reply[slot // (LEVELS * SLOTS)].astype(jnp.int32)
                    turned = pltpu.roll(block, QUERIES, 1)
                    halves.append(jnp.where(slot % SLOTS == side, block, turned))
                both = jnp.where(low, halves[0], halves[1]).astype(jnp.float32)
                power = both[LEVELS * WINDOW + level : LEVELS * WINDOW + level + 1]
                factor = jnp.exp2(power) * (scale / FULL)
                values = both[level * WINDOW : (level + 1) * WINDOW] * factor
                out[:, level, group * LANES : (group + 1) * LANES] = values

    return kernel


def steps(fmap1, fmap2, target_owner, target_tile):
    frames, band_rows, band_cols, channels = fmap1.shape
    peers = lax.axis_size("rows") * lax.axis_size("cols")
    across = band_cols // SIDE
    per_frame = band_rows // SIDE * across
    blocks = frames * per_frame
    across_of = [(band_cols >> l) // SIDE for l in range(LEVELS)]
    tiles_of = [((band_rows >> l) // SIDE) * across_of[l] for l in range(LEVELS)]

    parts = LEVELS * SLOTS * SIDE + 1
    smem = pl.BlockSpec(memory_space=pltpu.SMEM)
    hbm = pl.BlockSpec(memory_space=pl.ANY)
    send, codes = pl.pallas_call(
        build_body(peers, blocks, tiles_of, per_frame, across, band_rows),
        in_specs=[smem, smem, pl.BlockSpec(memory_space=pltpu.VMEM)],
        out_specs=[hbm, smem],
        out_shape=[
            jax.ShapeDtypeStruct((peers, parts, SIDE, channels), jnp.bfloat16),
            jax.ShapeDtypeStruct((LEVELS * blocks,), jnp.int32),
        ],
        scratch_shapes=[
            pltpu.SMEM((LEVELS * peers,), jnp.int32),
            pltpu.SMEM((LEVELS * SLOTS * peers,), jnp.int32),
            pltpu.VMEM((peers, SIDE, channels), jnp.bfloat16),
            pltpu.SemaphoreType.DMA((LEVELS * blocks,)),
            pltpu.SemaphoreType.DMA,
        ],
        name="build",
    )(
        target_owner.transpose(0, 2, 1),
        target_tile,
        fmap1.reshape(frames * band_rows, across, SIDE, channels),
    )

    def exchange(value):
        return lax.all_to_all(value, AXES, split_axis=0, concat_axis=0, tiled=True)

    arrived = exchange(send.reshape(peers, parts * SIDE, channels))

    low, high = neighbours(fmap2, "rows", 1, SIDE)
    edges = [
        jnp.concatenate([lax.slice_in_dim(part, *span, axis=2) for part in (low, fmap2, high)], axis=1)
        for span in ((0, SIDE), (band_cols - SIDE, band_cols))
    ]
    west, east = swapped(edges[1], edges[0], "cols")
    tall = jnp.concatenate([low, fmap2, high], axis=1)
    wide = jnp.concatenate([west, tall, east], axis=2)
    maps = [wide[:, RADIUS:-RADIUS, RADIUS:-RADIUS], pool_level(wide)]
    strips = [window_strips(level_map) for level_map in maps]

    rows_sent = LEVELS * LANES
    served = pl.pallas_call(
        serve_body([m.shape[1] for m in maps], across_of, tiles_of, frames, peers),
        grid=(peers // PEERS_A_STEP,),
        in_specs=[
            pl.BlockSpec((peers, SIDE, channels), lambda s: (0, rows_sent // SIDE, 0)),
            pl.BlockSpec((PEERS_A_STEP, rows_sent, channels), lambda s: (s, 0, 0)),
            pl.BlockSpec(strips[0].shape, lambda s: (0, 0, 0)),
            pl.BlockSpec(strips[1].shape, lambda s: (0, 0, 0)),
        ],
        out_specs=pl.BlockSpec((PEERS_A_STEP, REPLY_ROWS, LANES), lambda s: (s, 0, 0)),
        scratch_shapes=[
            pltpu.VMEM((BENCHES, REPLY_ROWS, LANES), jnp.float32),
            pltpu.VMEM((peers, 128), jnp.int32),
            pltpu.SMEM((peers, 128), jnp.int32),
            pltpu.SemaphoreType.DMA,
        ],
        out_shape=jax.ShapeDtypeStruct((peers, REPLY_ROWS, LANES), jnp.int16),
        name="serve",
    )(arrived, arrived, *strips)
    reply = exchange(served)

    groups = 4
    width = groups * LANES
    out = pl.pallas_call(
        finish_body(blocks, groups, channels ** (-0.5)),
        grid_spec=pltpu.PrefetchScalarGridSpec(
            num_scalar_prefetch=1,
            grid=(blocks * QUERIES // width,),
            in_specs=[pl.BlockSpec((peers, REPLY_ROWS, LANES), lambda s, _: (0, 0, 0))],
            out_specs=pl.BlockSpec((WINDOW, LEVELS, width), lambda s, _: (0, 0, s)),
        ),
        out_shape=jax.ShapeDtypeStruct((WINDOW, LEVELS, blocks * QUERIES), jnp.float32),
        name="finish",
    )(codes, reply)
    return out.transpose(1, 0, 2)


def solution(mesh):
    in_specs = (
        P(None, "rows", "cols", None),
        P(None, "rows", "cols", None),
        P(None, AXES, None),
        P(None, AXES),
    )
    out_specs = P(None, None, AXES)
    return jax.shard_map(steps, mesh=mesh, in_specs=in_specs, out_specs=out_specs, check_vma=False)
```

```python
import jax
import jax.numpy as jnp
from jax import lax
from jax.experimental import pallas as pl
from jax.experimental.pallas import tpu as pltpu
from jax.sharding import PartitionSpec as P


RADIUS = 4
LEVELS = 2
SIDE = 2 * RADIUS
SPAN = 4 * RADIUS
WIN = 2 * RADIUS + 1
WINDOW = WIN * WIN
QUERIES = SIDE * SIDE
SLOTS = 2
LANES = SLOTS * QUERIES
REPLY_ROWS = -(-(WINDOW + 1) // 8) * 8
PEERS_A_STEP = 16
BENCHES = 4
FULL = 32767.0
AXES = ("rows", "cols")


def swapped(upward, downward, axis):
    count = lax.axis_size(axis)
    forward = [(i, i + 1) for i in range(count - 1)]
    backward = [(target, source) for source, target in forward]
    return lax.ppermute(upward, axis, forward), lax.ppermute(downward, axis, backward)


def neighbours(block, axis, dim, width):
    tail = lax.slice_in_dim(block, block.shape[dim] - width, None, axis=dim)
    return swapped(tail, lax.slice_in_dim(block, 0, width, axis=dim), axis)


def pool_level(level_map):
    frame_count, rows_in, cols_in, channels = level_map.shape
    pooled = level_map.astype(jnp.float32).reshape(
        frame_count, rows_in // 2, 2, cols_in // 2, 2, channels
    )
    return jnp.mean(pooled, axis=(2, 4)).astype(jnp.bfloat16)


def window_strips(padded):
    frames, rows, cols, channels = padded.shape
    across = (cols - SIDE) // SIDE
    strips = [
        lax.slice_in_dim(padded, t * SIDE, t * SIDE + SPAN, axis=2) for t in range(across)
    ]
    return jnp.stack(strips).reshape(across * frames * rows, SPAN, channels)


def tile_copy(fmap, send, sems, per_frame, across, band_rows):
    def copy(k, slot):
        frame = k // per_frame
        rest = k % per_frame
        row = frame * band_rows + rest // across * SIDE
        return pltpu.make_async_copy(
            fmap.at[pl.ds(row, SIDE), rest % across],
            send.at[slot // SLOTS, pl.ds(slot % SLOTS * SIDE, SIDE)],
            sems.at[k],
        )

    return copy


def first_body(peers, blocks, tiles_of, per_frame, across, band_rows):
    last = LEVELS - 1

    def kernel(owner, tile, fmap, send, slots, count, labels, notes, sems, note_sem):
        copy = tile_copy(fmap, send, sems, per_frame, across, band_rows)

        def clear(i, carry):
            count[i] = 0
            return carry

        lax.fori_loop(0, LEVELS * peers, clear, 0, unroll=8)

        def blank(i, carry):
            labels[i] = 0
            return carry

        lax.fori_loop(0, LEVELS * SLOTS * peers, blank, 0, unroll=8)

        def place(k, carry):
            for level in reversed(range(LEVELS)):
                own = owner[level, 0, k]
                seen = count[level * peers + own]
                count[level * peers + own] = seen + 1
                slot = own * SLOTS + seen
                slots[level * blocks + k] = slot
                labels[level * SLOTS * peers + slot] = k // per_frame * tiles_of[level] + lax.rem(
                    tile[level, k], tiles_of[level]
                )
                if level == last:
                    copy(k, slot).start()
            return carry

        lax.fori_loop(0, blocks, place, 0)

        lane = lax.broadcasted_iota(jnp.int32, notes.shape[1:], 1)

        def note(peer, carry):
            values = jnp.zeros(notes.shape[1:], jnp.int32)
            for level in range(LEVELS):
                for seen in range(SLOTS):
                    label = labels[(level * peers + peer) * SLOTS + seen]
                    values = jnp.where(lane == level * SLOTS + seen, label, values)
            notes[peer] = values.astype(jnp.float32).astype(jnp.bfloat16)
            return carry

        lax.fori_loop(0, peers, note, 0, unroll=4)
        noted = pltpu.make_async_copy(notes, send.at[:, SLOTS * SIDE], note_sem)
        noted.start()

        def finish(k, carry):
            copy(k, slots[last * blocks + k]).wait()
            return carry

        lax.fori_loop(0, blocks, finish, 0)
        noted.wait()

    return kernel


def second_body(blocks, per_frame, across, band_rows):
    def kernel(slots, fmap, send, sems):
        copy = tile_copy(fmap, send, sems, per_frame, across, band_rows)

        def place(k, carry):
            copy(k, slots[k]).start()
            return carry

        def finish(k, carry):
            copy(k, slots[k]).wait()
            return carry

        lax.fori_loop(0, blocks, place, 0)
        lax.fori_loop(0, blocks, finish, 0)

    return kernel


def serve_body(level, rows, across, tiles, frames, peers):
    def kernel(notes, queries, strips, reply, flat, lines, labels, sem):
        step = pl.program_id(0)
        lane = lax.broadcasted_iota(jnp.int32, (1, LANES), 1)
        first = lane < QUERIES
        i_part = lane % QUERIES // SIDE
        j_part = lane % SIDE
        row_id = lax.broadcasted_iota(jnp.int32, (REPLY_ROWS, LANES), 0)

        @pl.when(step == 0)
        def _():
            flat[...] = jnp.zeros_like(flat)

            def line(peer, carry):
                values = notes[peer].astype(jnp.float32).astype(jnp.int32)
                lines[pl.ds(peer, 1), :] = values[:1, : lines.shape[1]]
                return carry

            lax.fori_loop(0, peers, line, 0, unroll=8)
            taken = pltpu.make_async_copy(lines, labels, sem)
            taken.start()
            taken.wait()

        def start_of(label):
            tile = label % tiles
            column = tile % across
            return (column * frames + label // tiles) * rows + tile // across * SIDE

        def one(peer, bench):
            query = queries[peer]
            tables = []
            for slot in range(SLOTS):
                label = labels[step * PEERS_A_STEP + peer, level * SLOTS + slot]
                cells = strips[pl.ds(start_of(label), SPAN)]
                tables.append(
                    lax.dot_general(
                        cells.reshape(SPAN * SPAN, -1),
                        query,
                        (((1,), (1,)), ((), ())),
                        preferred_element_type=jnp.float32,
                    )
                )
            table = jnp.where(first, tables[0], tables[1])
            table = table.reshape(SPAN, SPAN, LANES)
            for bit in (4, 2, 1):
                left = table.shape[0] - bit
                table = jnp.where(i_part & bit != 0, table[bit:], table[:left])
            table = table.reshape(WIN * SPAN, LANES)
            for bit in (4, 2, 1):
                table = jnp.where(
                    j_part & bit != 0, pltpu.roll(table, WIN * SPAN - bit, 0), table
                )
            for a in range(WIN):
                flat[bench, a * WIN : (a + 1) * WIN, :] = table[a * SPAN : a * SPAN + WIN]
            values = flat[bench]
            top = jnp.max(jnp.abs(values), axis=0, keepdims=True)
            power = jnp.ceil(jnp.log2(jnp.maximum(top, 1e-30)))
            coded = jnp.round(values * (jnp.exp2(-power) * FULL))
            coded = jnp.clip(coded, -FULL, FULL)
            coded = jnp.where(row_id == WINDOW, power, coded)
            reply[peer] = coded.astype(jnp.int32).astype(jnp.int16)

        def turn(i, carry):
            for bench in range(BENCHES):
                one(i * BENCHES + bench, bench)
            return carry

        lax.fori_loop(0, PEERS_A_STEP // BENCHES, turn, 0)

    return kernel


def finish_body(blocks, groups, scale):
    def kernel(slots, reply0, reply1, out):
        step = pl.program_id(0)
        low = lax.broadcasted_iota(jnp.int32, (1, LANES), 1) < QUERIES
        for level, reply in enumerate((reply0, reply1)):
            for group in range(groups):
                k = level * blocks + (step * groups + group) * 2
                halves = []
                for side in range(2):
                    slot = slots[k + side]
                    block = reply[slot // SLOTS].astype(jnp.int32)
                    turned = pltpu.roll(block, QUERIES, 1)
                    halves.append(jnp.where(slot % SLOTS == side, block, turned))
                both = jnp.where(low, halves[0], halves[1]).astype(jnp.float32)
                factor = jnp.exp2(both[WINDOW : WINDOW + 1]) * (scale / FULL)
                out[:, level, group * LANES : (group + 1) * LANES] = both[:WINDOW] * factor

    return kernel


def steps(fmap1, fmap2, target_owner, target_tile):
    frames, band_rows, band_cols, channels = fmap1.shape
    peers = lax.axis_size("rows") * lax.axis_size("cols")
    across = band_cols // SIDE
    per_frame = band_rows // SIDE * across
    blocks = frames * per_frame
    across_of = [(band_cols >> l) // SIDE for l in range(LEVELS)]
    tiles_of = [((band_rows >> l) // SIDE) * across_of[l] for l in range(LEVELS)]

    smem = pl.BlockSpec(memory_space=pltpu.SMEM)
    vmem = pl.BlockSpec(memory_space=pltpu.VMEM)
    hbm = pl.BlockSpec(memory_space=pl.ANY)
    tiles = fmap1.reshape(frames * band_rows, across, SIDE, channels)

    def send_shape(parts):
        return jax.ShapeDtypeStruct((peers, parts, SIDE, channels), jnp.bfloat16)

    send1, slots = pl.pallas_call(
        first_body(peers, blocks, tiles_of, per_frame, across, band_rows),
        in_specs=[smem, smem, vmem],
        out_specs=[hbm, smem],
        out_shape=[
            send_shape(SLOTS * SIDE + 1),
            jax.ShapeDtypeStruct((LEVELS * blocks,), jnp.int32),
        ],
        scratch_shapes=[
            pltpu.SMEM((LEVELS * peers,), jnp.int32),
            pltpu.SMEM((LEVELS * SLOTS * peers,), jnp.int32),
            pltpu.VMEM((peers, SIDE, channels), jnp.bfloat16),
            pltpu.SemaphoreType.DMA((blocks,)),
            pltpu.SemaphoreType.DMA,
        ],
        name="build1",
    )(target_owner.transpose(0, 2, 1), target_tile, tiles)
    send0 = pl.pallas_call(
        second_body(blocks, per_frame, across, band_rows),
        in_specs=[smem, vmem],
        out_specs=hbm,
        out_shape=send_shape(SLOTS * SIDE),
        scratch_shapes=[pltpu.SemaphoreType.DMA((blocks,))],
        name="build0",
    )(slots, tiles)

    def exchange(value):
        return lax.all_to_all(value, AXES, split_axis=0, concat_axis=0, tiled=True)

    arrived = [exchange(send.reshape(peers, -1, channels)) for send in (send0, send1)]

    low, high = neighbours(fmap2, "rows", 1, SIDE)
    edges = [
        jnp.concatenate([lax.slice_in_dim(part, *span, axis=2) for part in (low, fmap2, high)], axis=1)
        for span in ((0, SIDE), (band_cols - SIDE, band_cols))
    ]
    west, east = swapped(edges[1], edges[0], "cols")
    tall = jnp.concatenate([low, fmap2, high], axis=1)
    wide = jnp.concatenate([west, tall, east], axis=2)
    maps = [wide[:, RADIUS:-RADIUS, RADIUS:-RADIUS], pool_level(wide)]

    replies = []
    for level in range(LEVELS):
        strips = window_strips(maps[level])
        served = pl.pallas_call(
            serve_body(level, maps[level].shape[1], across_of[level], tiles_of[level], frames, peers),
            grid=(peers // PEERS_A_STEP,),
            in_specs=[
                pl.BlockSpec((peers, SIDE, channels), lambda s: (0, LANES // SIDE, 0)),
                pl.BlockSpec((PEERS_A_STEP, LANES, channels), lambda s: (s, 0, 0)),
                pl.BlockSpec(strips.shape, lambda s: (0, 0, 0)),
            ],
            out_specs=pl.BlockSpec((PEERS_A_STEP, REPLY_ROWS, LANES), lambda s: (s, 0, 0)),
            scratch_shapes=[
                pltpu.VMEM((BENCHES, REPLY_ROWS, LANES), jnp.float32),
                pltpu.VMEM((peers, 128), jnp.int32),
                pltpu.SMEM((peers, 128), jnp.int32),
                pltpu.SemaphoreType.DMA,
            ],
            out_shape=jax.ShapeDtypeStruct((peers, REPLY_ROWS, LANES), jnp.int16),
        )(arrived[1], arrived[level], strips)
        replies.append(exchange(served))

    groups = 4
    width = groups * LANES
    whole = pl.BlockSpec((peers, REPLY_ROWS, LANES), lambda s, _: (0, 0, 0))
    out = pl.pallas_call(
        finish_body(blocks, groups, channels ** (-0.5)),
        grid_spec=pltpu.PrefetchScalarGridSpec(
            num_scalar_prefetch=1,
            grid=(blocks * QUERIES // width,),
            in_specs=[whole, whole],
            out_specs=pl.BlockSpec((WINDOW, LEVELS, width), lambda s, _: (0, 0, s)),
        ),
        out_shape=jax.ShapeDtypeStruct((WINDOW, LEVELS, blocks * QUERIES), jnp.float32),
        name="finish",
    )(slots, *replies)
    return out.transpose(1, 0, 2)


def solution(mesh):
    in_specs = (
        P(None, "rows", "cols", None),
        P(None, "rows", "cols", None),
        P(None, AXES, None),
        P(None, AXES),
    )
    out_specs = P(None, None, AXES)
    return jax.shard_map(steps, mesh=mesh, in_specs=in_specs, out_specs=out_specs, check_vma=False)
```

```python
import jax
import jax.numpy as jnp
from jax import lax
from jax.experimental import pallas as pl
from jax.experimental.pallas import tpu as pltpu
from jax.sharding import PartitionSpec as P


RADIUS = 4
LEVELS = 2
SIDE = 2 * RADIUS
SPAN = 4 * RADIUS
WIN = 2 * RADIUS + 1
WINDOW = WIN * WIN
QUERIES = SIDE * SIDE
SLOTS = 2
LANES = SLOTS * QUERIES
REPLY_ROWS = -(-(WINDOW + 1) // 8) * 8
PEERS_A_STEP = 16
BENCHES = 8
FULL = 32767.0
AXES = ("rows", "cols")


def halo(block, width):
    sizes = [lax.axis_size(axis) for axis in AXES]
    rows, cols = block.shape[1:3]

    def side(step, extent):
        return {0: (0, extent), 1: (extent - width, extent), -1: (0, width)}[step]

    def from_neighbour(down, right):
        piece = block[:, slice(*side(down, rows)), slice(*side(right, cols))]
        pairs = [
            (r * sizes[1] + c, (r + down) * sizes[1] + c + right)
            for r in range(sizes[0])
            for c in range(sizes[1])
            if 0 <= r + down < sizes[0] and 0 <= c + right < sizes[1]
        ]
        return lax.ppermute(piece, AXES, pairs)

    bands = []
    for down in (1, 0, -1):
        band = [
            block if down == right == 0 else from_neighbour(down, right) for right in (1, 0, -1)
        ]
        bands.append(jnp.concatenate(band, axis=2))
    return jnp.concatenate(bands, axis=1)


def pool_level(level_map):
    frame_count, rows_in, cols_in, channels = level_map.shape
    pooled = level_map.astype(jnp.float32).reshape(
        frame_count, rows_in // 2, 2, cols_in // 2, 2, channels
    )
    return jnp.mean(pooled, axis=(2, 4)).astype(jnp.bfloat16)


def window_strips(padded):
    frames, rows, cols, channels = padded.shape
    across = (cols - SIDE) // SIDE
    strips = [
        lax.slice_in_dim(padded, t * SIDE, t * SIDE + SPAN, axis=2) for t in range(across)
    ]
    return jnp.stack(strips).reshape(across * frames * rows, SPAN, channels)


def tile_copy(fmap, send, sems, per_frame, across, band_rows):
    def copy(k, slot):
        frame = k // per_frame
        rest = k % per_frame
        row = frame * band_rows + rest // across * SIDE
        return pltpu.make_async_copy(
            fmap.at[pl.ds(row, SIDE), rest % across],
            send.at[slot // SLOTS, pl.ds(slot % SLOTS * SIDE, SIDE)],
            sems.at[k],
        )

    return copy


def first_body(peers, blocks, tiles_of, per_frame, across, band_rows):
    last = LEVELS - 1

    def kernel(owner, tile, fmap, send, slots, count, labels, notes, sems, note_sem):
        copy = tile_copy(fmap, send, sems, per_frame, across, band_rows)

        def clear(i, carry):
            count[i] = 0
            return carry

        lax.fori_loop(0, LEVELS * peers, clear, 0, unroll=8)

        def blank(i, carry):
            labels[i] = 0
            return carry

        lax.fori_loop(0, LEVELS * SLOTS * peers, blank, 0, unroll=8)

        def place(k, carry):
            for level in reversed(range(LEVELS)):
                own = owner[level, 0, k]
                seen = count[level * peers + own]
                count[level * peers + own] = seen + 1
                slot = own * SLOTS + seen
                slots[level * blocks + k] = slot
                labels[level * SLOTS * peers + slot] = k // per_frame * tiles_of[level] + lax.rem(
                    tile[level, k], tiles_of[level]
                )
                if level == last:
                    copy(k, slot).start()
            return carry

        lax.fori_loop(0, blocks, place, 0)

        lane = lax.broadcasted_iota(jnp.int32, notes.shape[1:], 1)

        def note(peer, carry):
            values = jnp.zeros(notes.shape[1:], jnp.int32)
            for level in range(LEVELS):
                for seen in range(SLOTS):
                    label = labels[(level * peers + peer) * SLOTS + seen]
                    values = jnp.where(lane == level * SLOTS + seen, label, values)
            notes[peer] = values.astype(jnp.float32).astype(jnp.bfloat16)
            return carry

        lax.fori_loop(0, peers, note, 0, unroll=4)
        noted = pltpu.make_async_copy(notes, send.at[:, SLOTS * SIDE], note_sem)
        noted.start()

        def finish(k, carry):
            copy(k, slots[last * blocks + k]).wait()
            return carry

        lax.fori_loop(0, blocks, finish, 0)
        noted.wait()

    return kernel


def second_body(blocks, per_frame, across, band_rows):
    def kernel(slots, fmap, send, sems):
        copy = tile_copy(fmap, send, sems, per_frame, across, band_rows)

        def place(k, carry):
            copy(k, slots[k]).start()
            return carry

        def finish(k, carry):
            copy(k, slots[k]).wait()
            return carry

        lax.fori_loop(0, blocks, place, 0)
        lax.fori_loop(0, blocks, finish, 0)

    return kernel


def serve_body(level, rows, across, tiles, frames, peers):
    def kernel(notes, queries, strips, reply, flat, lines, labels, sem):
        step = pl.program_id(0)
        lane = lax.broadcasted_iota(jnp.int32, (1, LANES), 1)
        first = lane < QUERIES
        i_part = lane % QUERIES // SIDE
        j_part = lane % SIDE
        row_id = lax.broadcasted_iota(jnp.int32, (REPLY_ROWS, LANES), 0)

        @pl.when(step == 0)
        def _():
            flat[...] = jnp.zeros_like(flat)

            def line(peer, carry):
                values = notes[peer].astype(jnp.float32).astype(jnp.int32)
                lines[pl.ds(peer, 1), :] = values[:1, : lines.shape[1]]
                return carry

            lax.fori_loop(0, peers, line, 0, unroll=8)
            taken = pltpu.make_async_copy(lines, labels, sem)
            taken.start()
            taken.wait()

        def start_of(label):
            tile = label % tiles
            column = tile % across
            return (column * frames + label // tiles) * rows + tile // across * SIDE

        def one(peer, bench):
            query = queries[peer]
            tables = []
            for slot in range(SLOTS):
                label = labels[step * PEERS_A_STEP + peer, level * SLOTS + slot]
                cells = strips[pl.ds(start_of(label), SPAN)]
                tables.append(
                    lax.dot_general(
                        cells.reshape(SPAN * SPAN, -1),
                        query,
                        (((1,), (1,)), ((), ())),
                        preferred_element_type=jnp.float32,
                    )
                )
            table = jnp.where(first, tables[0], tables[1])
            table = table.reshape(SPAN, SPAN, LANES)
            for bit in (4, 2, 1):
                left = table.shape[0] - bit
                table = jnp.where(i_part & bit != 0, table[bit:], table[:left])
            table = table.reshape(WIN * SPAN, LANES)
            for bit in (4, 2, 1):
                table = jnp.where(
                    j_part & bit != 0, pltpu.roll(table, WIN * SPAN - bit, 0), table
                )
            for a in range(WIN):
                flat[bench, a * WIN : (a + 1) * WIN, :] = table[a * SPAN : a * SPAN + WIN]
            values = flat[bench]
            top = jnp.max(jnp.abs(values), axis=0, keepdims=True)
            power = jnp.ceil(jnp.log2(jnp.maximum(top, 1e-30)))
            coded = jnp.round(values * (jnp.exp2(-power) * FULL))
            coded = jnp.clip(coded, -FULL, FULL)
            coded = jnp.where(row_id == WINDOW, power, coded)
            reply[peer] = coded.astype(jnp.int32).astype(jnp.int16)

        def turn(i, carry):
            for bench in range(BENCHES):
                one(i * BENCHES + bench, bench)
            return carry

        lax.fori_loop(0, PEERS_A_STEP // BENCHES, turn, 0)

    return kernel


def finish_body(blocks, groups, scale):
    def kernel(slots, reply0, reply1, out):
        step = pl.program_id(0)
        low = lax.broadcasted_iota(jnp.int32, (1, LANES), 1) < QUERIES
        for level, reply in enumerate((reply0, reply1)):
            for group in range(groups):
                k = level * blocks + (step * groups + group) * 2
                slot = [slots[k + side] for side in range(2)]
                block = [reply[at // SLOTS].astype(jnp.int32) for at in slot]
                straight = jnp.where(low, block[0], block[1])
                turned = pltpu.roll(jnp.where(low, block[1], block[0]), QUERIES, 1)
                kept = [slot[side] % SLOTS == side for side in range(2)]
                left = jnp.where(kept[0], straight, turned)
                right = jnp.where(kept[1], straight, turned)
                both = jnp.where(low, left, right).astype(jnp.float32)
                factor = jnp.exp2(both[WINDOW : WINDOW + 1]) * (scale / FULL)
                out[:, level, group * LANES : (group + 1) * LANES] = both[:WINDOW] * factor

    return kernel


def steps(fmap1, fmap2, target_owner, target_tile):
    frames, band_rows, band_cols, channels = fmap1.shape
    peers = lax.axis_size("rows") * lax.axis_size("cols")
    across = band_cols // SIDE
    per_frame = band_rows // SIDE * across
    blocks = frames * per_frame
    across_of = [(band_cols >> l) // SIDE for l in range(LEVELS)]
    tiles_of = [((band_rows >> l) // SIDE) * across_of[l] for l in range(LEVELS)]

    smem = pl.BlockSpec(memory_space=pltpu.SMEM)
    vmem = pl.BlockSpec(memory_space=pltpu.VMEM)
    hbm = pl.BlockSpec(memory_space=pl.ANY)
    tiles = fmap1.reshape(frames * band_rows, across, SIDE, channels)

    def send_shape(parts):
        return jax.ShapeDtypeStruct((peers, parts, SIDE, channels), jnp.bfloat16)

    send1, slots = pl.pallas_call(
        first_body(peers, blocks, tiles_of, per_frame, across, band_rows),
        in_specs=[smem, smem, vmem],
        out_specs=[hbm, smem],
        out_shape=[
            send_shape(SLOTS * SIDE + 1),
            jax.ShapeDtypeStruct((LEVELS * blocks,), jnp.int32),
        ],
        scratch_shapes=[
            pltpu.SMEM((LEVELS * peers,), jnp.int32),
            pltpu.SMEM((LEVELS * SLOTS * peers,), jnp.int32),
            pltpu.VMEM((peers, SIDE, channels), jnp.bfloat16),
            pltpu.SemaphoreType.DMA((blocks,)),
            pltpu.SemaphoreType.DMA,
        ],
        name="build1",
    )(target_owner.transpose(0, 2, 1), target_tile, tiles)
    send0 = pl.pallas_call(
        second_body(blocks, per_frame, across, band_rows),
        in_specs=[smem, vmem],
        out_specs=hbm,
        out_shape=send_shape(SLOTS * SIDE),
        scratch_shapes=[pltpu.SemaphoreType.DMA((blocks,))],
        name="build0",
    )(slots, tiles)

    def exchange(value):
        return lax.all_to_all(value, AXES, split_axis=0, concat_axis=0, tiled=True)

    arrived = [exchange(send.reshape(peers, -1, channels)) for send in (send0, send1)]

    wide = halo(fmap2, SIDE)
    maps = [wide[:, RADIUS:-RADIUS, RADIUS:-RADIUS], pool_level(wide)]

    replies = []
    for level in range(LEVELS):
        strips = window_strips(maps[level])
        served = pl.pallas_call(
            serve_body(level, maps[level].shape[1], across_of[level], tiles_of[level], frames, peers),
            grid=(peers // PEERS_A_STEP,),
            in_specs=[
                pl.BlockSpec((peers, SIDE, channels), lambda s: (0, LANES // SIDE, 0)),
                pl.BlockSpec((PEERS_A_STEP, LANES, channels), lambda s: (s, 0, 0)),
                pl.BlockSpec(strips.shape, lambda s: (0, 0, 0)),
            ],
            out_specs=pl.BlockSpec((PEERS_A_STEP, REPLY_ROWS, LANES), lambda s: (s, 0, 0)),
            scratch_shapes=[
                pltpu.VMEM((BENCHES, REPLY_ROWS, LANES), jnp.float32),
                pltpu.VMEM((peers, 128), jnp.int32),
                pltpu.SMEM((peers, 128), jnp.int32),
                pltpu.SemaphoreType.DMA,
            ],
            out_shape=jax.ShapeDtypeStruct((peers, REPLY_ROWS, LANES), jnp.int16),
        )(arrived[1], arrived[level], strips)
        replies.append(exchange(served))

    groups = 4
    width = groups * LANES
    whole = pl.BlockSpec((peers, REPLY_ROWS, LANES), lambda s, _: (0, 0, 0))
    out = pl.pallas_call(
        finish_body(blocks, groups, channels ** (-0.5)),
        grid_spec=pltpu.PrefetchScalarGridSpec(
            num_scalar_prefetch=1,
            grid=(blocks * QUERIES // width,),
            in_specs=[whole, whole],
            out_specs=pl.BlockSpec((WINDOW, LEVELS, width), lambda s, _: (0, 0, s)),
        ),
        out_shape=jax.ShapeDtypeStruct((WINDOW, LEVELS, blocks * QUERIES), jnp.float32),
        name="finish",
    )(slots, *replies)
    return out.transpose(1, 0, 2)


def solution(mesh):
    in_specs = (
        P(None, "rows", "cols", None),
        P(None, "rows", "cols", None),
        P(None, AXES, None),
        P(None, AXES),
    )
    out_specs = P(None, None, AXES)
    return jax.shard_map(steps, mesh=mesh, in_specs=in_specs, out_specs=out_specs, check_vma=False)
```

```python
import jax
import jax.numpy as jnp
from jax import lax
from jax.experimental import pallas as pl
from jax.experimental.pallas import tpu as pltpu
from jax.sharding import PartitionSpec as P


RADIUS = 4
LEVELS = 2
SIDE = 2 * RADIUS
SPAN = 4 * RADIUS
WIN = 2 * RADIUS + 1
WINDOW = WIN * WIN
QUERIES = SIDE * SIDE
SLOTS = 2
LANES = SLOTS * QUERIES
PART_ROWS = 88
EARLY_ROWS = 80
REPLY_ROWS = EARLY_ROWS + PART_ROWS
PEERS_A_STEP = 16
BENCHES = 8
FULL = 32767.0
AXES = ("rows", "cols")


def swapped(upward, downward, axis):
    count = lax.axis_size(axis)
    forward = [(i, i + 1) for i in range(count - 1)]
    backward = [(target, source) for source, target in forward]
    return lax.ppermute(upward, axis, forward), lax.ppermute(downward, axis, backward)


def neighbours(block, axis, dim, width):
    tail = lax.slice_in_dim(block, block.shape[dim] - width, None, axis=dim)
    return swapped(tail, lax.slice_in_dim(block, 0, width, axis=dim), axis)


def pool_level(level_map):
    frame_count, rows_in, cols_in, channels = level_map.shape
    pooled = level_map.astype(jnp.float32).reshape(
        frame_count, rows_in // 2, 2, cols_in // 2, 2, channels
    )
    return jnp.mean(pooled, axis=(2, 4)).astype(jnp.bfloat16)


def window_strips(padded):
    frames, rows, cols, channels = padded.shape
    across = (cols - SIDE) // SIDE
    strips = [
        lax.slice_in_dim(padded, t * SIDE, t * SIDE + SPAN, axis=2) for t in range(across)
    ]
    return jnp.stack(strips).reshape(across * frames * rows, SPAN, channels)


def tile_copy(fmap, send, sems, per_frame, across, band_rows):
    def copy(k, slot):
        frame = k // per_frame
        rest = k % per_frame
        row = frame * band_rows + rest // across * SIDE
        return pltpu.make_async_copy(
            fmap.at[pl.ds(row, SIDE), rest % across],
            send.at[slot // SLOTS, pl.ds(slot % SLOTS * SIDE, SIDE)],
            sems.at[k],
        )

    return copy


def first_body(peers, blocks, tiles_of, per_frame, across, band_rows):
    last = LEVELS - 1

    def kernel(owner, tile, fmap, send, slots, count, labels, notes, sems, note_sem):
        copy = tile_copy(fmap, send, sems, per_frame, across, band_rows)

        def clear(i, carry):
            count[i] = 0
            return carry

        lax.fori_loop(0, LEVELS * peers, clear, 0, unroll=8)

        def blank(i, carry):
            labels[i] = 0
            return carry

        lax.fori_loop(0, LEVELS * SLOTS * peers, blank, 0, unroll=8)

        def place(k, carry):
            for level in reversed(range(LEVELS)):
                own = owner[level, 0, k]
                seen = count[level * peers + own]
                count[level * peers + own] = seen + 1
                slot = own * SLOTS + seen
                slots[level * blocks + k] = slot
                labels[level * SLOTS * peers + slot] = k // per_frame * tiles_of[level] + lax.rem(
                    tile[level, k], tiles_of[level]
                )
                if level == last:
                    copy(k, slot).start()
            return carry

        lax.fori_loop(0, blocks, place, 0)

        lane = lax.broadcasted_iota(jnp.int32, notes.shape[1:], 1)

        def note(peer, carry):
            values = jnp.zeros(notes.shape[1:], jnp.int32)
            for level in range(LEVELS):
                for seen in range(SLOTS):
                    label = labels[(level * peers + peer) * SLOTS + seen]
                    values = jnp.where(lane == level * SLOTS + seen, label, values)
            notes[peer] = values.astype(jnp.float32).astype(jnp.bfloat16)
            return carry

        lax.fori_loop(0, peers, note, 0, unroll=4)
        noted = pltpu.make_async_copy(notes, send.at[:, SLOTS * SIDE], note_sem)
        noted.start()

        def finish(k, carry):
            copy(k, slots[last * blocks + k]).wait()
            return carry

        lax.fori_loop(0, blocks, finish, 0)
        noted.wait()

    return kernel


def second_body(blocks, per_frame, across, band_rows):
    def kernel(slots, fmap, send, sems):
        copy = tile_copy(fmap, send, sems, per_frame, across, band_rows)

        def place(k, carry):
            copy(k, slots[k]).start()
            return carry

        def finish(k, carry):
            copy(k, slots[k]).wait()
            return carry

        lax.fori_loop(0, blocks, place, 0)
        lax.fori_loop(0, blocks, finish, 0)

    return kernel


def window_table(query, cells, first, i_part, j_part):
    tables = [
        lax.dot_general(
            window.reshape(SPAN * SPAN, -1),
            query,
            (((1,), (1,)), ((), ())),
            preferred_element_type=jnp.float32,
        )
        for window in cells
    ]
    table = jnp.where(first, tables[0], tables[1]).reshape(SPAN, SPAN, LANES)
    for bit in (4, 2, 1):
        left = table.shape[0] - bit
        table = jnp.where(i_part & bit != 0, table[bit:], table[:left])
    table = table.reshape(WIN * SPAN, LANES)
    for bit in (4, 2, 1):
        table = jnp.where(j_part & bit != 0, pltpu.roll(table, WIN * SPAN - bit, 0), table)
    return table


def serve_body(rows, across, tiles, frames, label_of):
    def run(step, queries, strips, flat, store):
        lane = lax.broadcasted_iota(jnp.int32, (1, LANES), 1)
        first = lane < QUERIES
        i_part = lane % QUERIES // SIDE
        j_part = lane % SIDE
        row_id = lax.broadcasted_iota(jnp.int32, (PART_ROWS, LANES), 0)

        def start_of(label):
            tile = label % tiles
            column = tile % across
            return (column * frames + label // tiles) * rows + tile // across * SIDE

        def one(peer, bench):
            cells = [
                strips[pl.ds(start_of(label_of(step * PEERS_A_STEP + peer, slot)), SPAN)]
                for slot in range(SLOTS)
            ]
            table = window_table(queries[peer], cells, first, i_part, j_part)
            for a in range(WIN):
                flat[bench, a * WIN : (a + 1) * WIN, :] = table[a * SPAN : a * SPAN + WIN]
            values = flat[bench]
            top = jnp.max(jnp.abs(values), axis=0, keepdims=True)
            power = jnp.ceil(jnp.log2(jnp.maximum(top, 1e-30)))
            coded = jnp.round(values * (jnp.exp2(-power) * FULL))
            coded = jnp.clip(coded, -FULL, FULL)
            store(peer, row_id, jnp.where(row_id == WINDOW, power, coded).astype(jnp.int32))

        def turn(i, carry):
            for bench in range(BENCHES):
                one(i * BENCHES + bench, bench)
            return carry

        lax.fori_loop(0, PEERS_A_STEP // BENCHES, turn, 0)

    return run


def serve1_body(rows, across, tiles, frames, peers):
    def kernel(notes, queries, strips, part, others, flat, lines, labels, sem):
        step = pl.program_id(0)

        @pl.when(step == 0)
        def _():
            flat[...] = jnp.zeros_like(flat)

            def line(peer, carry):
                values = notes[peer].astype(jnp.float32).astype(jnp.int32)
                lines[pl.ds(peer, 1), :] = values[:1, : lines.shape[1]]
                return carry

            lax.fori_loop(0, peers, line, 0, unroll=8)
            taken = pltpu.make_async_copy(lines, labels, sem)
            taken.start()
            taken.wait()

            def other(peer, carry):
                for slot in range(SLOTS):
                    others[peer * SLOTS + slot] = labels[peer, slot]
                return carry

            lax.fori_loop(0, peers, other, 0, unroll=4)

        def store(peer, row_id, coded):
            part[peer] = coded.astype(jnp.int16)

        run = serve_body(rows, across, tiles, frames, lambda p, slot: labels[p, SLOTS + slot])
        run(step, queries, strips, flat, store)

    return kernel


def serve0_body(rows, across, tiles, frames):
    def kernel(labels, queries, strips, part, reply, flat):
        step = pl.program_id(0)

        @pl.when(step == 0)
        def _():
            flat[...] = jnp.zeros_like(flat)

        def store(peer, row_id, coded):
            rest = part[peer, EARLY_ROWS:PART_ROWS].astype(jnp.int32)
            coded = jnp.where(row_id == WINDOW + 1, rest[0:1], coded)
            coded = jnp.where(row_id == WINDOW + 2, rest[1:2], coded)
            reply[peer, :EARLY_ROWS] = part[peer, :EARLY_ROWS]
            reply[peer, EARLY_ROWS:] = coded.astype(jnp.int16)

        run = serve_body(rows, across, tiles, frames, lambda p, slot: labels[p * SLOTS + slot])
        run(step, queries, strips, flat, store)

    return kernel


def finish_body(blocks, groups, scale):
    def kernel(slots, reply, out):
        step = pl.program_id(0)
        low = lax.broadcasted_iota(jnp.int32, (1, LANES), 1) < QUERIES

        def joined(slot, begin, end):
            block = [reply[at // SLOTS, begin:end].astype(jnp.int32) for at in slot]
            straight = jnp.where(low, block[0], block[1])
            turned = pltpu.roll(jnp.where(low, block[1], block[0]), QUERIES, 1)
            kept = [slot[side] % SLOTS == side for side in range(2)]
            left = jnp.where(kept[0], straight, turned)
            right = jnp.where(kept[1], straight, turned)
            return jnp.where(low, left, right).astype(jnp.float32)

        def unit(power):
            return jnp.exp2(power) * (scale / FULL)

        for group in range(groups):
            k = (step * groups + group) * 2
            lanes = slice(group * LANES, (group + 1) * LANES)
            late = joined([slots[k], slots[k + 1]], EARLY_ROWS, REPLY_ROWS)
            out[:, 0, lanes] = late[:WINDOW] * unit(late[WINDOW : WINDOW + 1])
            slot = [slots[blocks + k], slots[blocks + k + 1]]
            early = joined(slot, 0, EARLY_ROWS)
            last = joined(slot, REPLY_ROWS - 8, REPLY_ROWS)
            at = WINDOW - EARLY_ROWS
            factor = unit(last[at + 2 : at + 3])
            out[:EARLY_ROWS, 1, lanes] = early * factor
            out[EARLY_ROWS:, 1, lanes] = last[at + 1 : at + 2] * factor

    return kernel


def steps(fmap1, fmap2, target_owner, target_tile):
    frames, band_rows, band_cols, channels = fmap1.shape
    peers = lax.axis_size("rows") * lax.axis_size("cols")
    across = band_cols // SIDE
    per_frame = band_rows // SIDE * across
    blocks = frames * per_frame
    across_of = [(band_cols >> l) // SIDE for l in range(LEVELS)]
    tiles_of = [((band_rows >> l) // SIDE) * across_of[l] for l in range(LEVELS)]

    smem = pl.BlockSpec(memory_space=pltpu.SMEM)
    vmem = pl.BlockSpec(memory_space=pltpu.VMEM)
    hbm = pl.BlockSpec(memory_space=pl.ANY)
    tiles = fmap1.reshape(frames * band_rows, across, SIDE, channels)

    def send_shape(parts):
        return jax.ShapeDtypeStruct((peers, parts, SIDE, channels), jnp.bfloat16)

    send1, slots = pl.pallas_call(
        first_body(peers, blocks, tiles_of, per_frame, across, band_rows),
        in_specs=[smem, smem, vmem],
        out_specs=[hbm, smem],
        out_shape=[
            send_shape(SLOTS * SIDE + 1),
            jax.ShapeDtypeStruct((LEVELS * blocks,), jnp.int32),
        ],
        scratch_shapes=[
            pltpu.SMEM((LEVELS * peers,), jnp.int32),
            pltpu.SMEM((LEVELS * SLOTS * peers,), jnp.int32),
            pltpu.VMEM((peers, SIDE, channels), jnp.bfloat16),
            pltpu.SemaphoreType.DMA((blocks,)),
            pltpu.SemaphoreType.DMA,
        ],
        name="build1",
    )(target_owner.transpose(0, 2, 1), target_tile, tiles)
    send0 = pl.pallas_call(
        second_body(blocks, per_frame, across, band_rows),
        in_specs=[smem, vmem],
        out_specs=hbm,
        out_shape=send_shape(SLOTS * SIDE),
        scratch_shapes=[pltpu.SemaphoreType.DMA((blocks,))],
        name="build0",
    )(slots, tiles)

    def exchange(value):
        return lax.all_to_all(value, AXES, split_axis=0, concat_axis=0, tiled=True)

    arrived = [exchange(send.reshape(peers, -1, channels)) for send in (send0, send1)]

    low, high = neighbours(fmap2, "rows", 1, SIDE)
    edges = [
        jnp.concatenate([lax.slice_in_dim(part, *span, axis=2) for part in (low, fmap2, high)], axis=1)
        for span in ((0, SIDE), (band_cols - SIDE, band_cols))
    ]
    west, east = swapped(edges[1], edges[0], "cols")
    tall = jnp.concatenate([low, fmap2, high], axis=1)
    wide = jnp.concatenate([west, tall, east], axis=2)
    maps = [wide[:, RADIUS:-RADIUS, RADIUS:-RADIUS], pool_level(wide)]

    strips = []
    for level in range(LEVELS):
        strips.append(window_strips(maps[level]))

    def facts(level):
        return maps[level].shape[1], across_of[level], tiles_of[level], frames

    grid = (peers // PEERS_A_STEP,)
    query_block = pl.BlockSpec((PEERS_A_STEP, LANES, channels), lambda s, *_: (s, 0, 0))
    part_block = pl.BlockSpec((PEERS_A_STEP, PART_ROWS, LANES), lambda s, *_: (s, 0, 0))
    flat = pltpu.VMEM((BENCHES, PART_ROWS, LANES), jnp.float32)

    def strip_block(level):
        return pl.BlockSpec(strips[level].shape, lambda s, *_: (0, 0, 0))

    part, labels0 = pl.pallas_call(
        serve1_body(*facts(1), peers),
        grid=grid,
        in_specs=[
            pl.BlockSpec((peers, SIDE, channels), lambda s: (0, LANES // SIDE, 0)),
            query_block,
            strip_block(1),
        ],
        out_specs=[part_block, smem],
        out_shape=[
            jax.ShapeDtypeStruct((peers, PART_ROWS, LANES), jnp.int16),
            jax.ShapeDtypeStruct((peers * SLOTS,), jnp.int32),
        ],
        scratch_shapes=[
            flat,
            pltpu.VMEM((peers, 128), jnp.int32),
            pltpu.SMEM((peers, 128), jnp.int32),
            pltpu.SemaphoreType.DMA,
        ],
        name="serve1",
    )(arrived[1], arrived[1], strips[1])
    served = pl.pallas_call(
        serve0_body(*facts(0)),
        grid_spec=pltpu.PrefetchScalarGridSpec(
            num_scalar_prefetch=1,
            grid=grid,
            in_specs=[query_block, strip_block(0), part_block],
            out_specs=pl.BlockSpec(
                (PEERS_A_STEP, REPLY_ROWS, LANES), lambda s, *_: (s, 0, 0)
            ),
            scratch_shapes=[flat],
        ),
        out_shape=jax.ShapeDtypeStruct((peers, REPLY_ROWS, LANES), jnp.int16),
        name="serve0",
    )(labels0, arrived[0], strips[0], part)
    reply = exchange(served)

    groups = 4
    width = groups * LANES
    whole = pl.BlockSpec((peers, REPLY_ROWS, LANES), lambda s, _: (0, 0, 0))
    out = pl.pallas_call(
        finish_body(blocks, groups, channels ** (-0.5)),
        grid_spec=pltpu.PrefetchScalarGridSpec(
            num_scalar_prefetch=1,
            grid=(blocks * QUERIES // width,),
            in_specs=[whole],
            out_specs=pl.BlockSpec((WINDOW, LEVELS, width), lambda s, _: (0, 0, s)),
        ),
        out_shape=jax.ShapeDtypeStruct((WINDOW, LEVELS, blocks * QUERIES), jnp.float32),
        name="finish",
    )(slots, reply)
    return out.transpose(1, 0, 2)


def solution(mesh):
    in_specs = (
        P(None, "rows", "cols", None),
        P(None, "rows", "cols", None),
        P(None, AXES, None),
        P(None, AXES),
    )
    out_specs = P(None, None, AXES)
    return jax.shard_map(steps, mesh=mesh, in_specs=in_specs, out_specs=out_specs, check_vma=False)
```

```python
import jax
import jax.numpy as jnp
from jax import lax
from jax.experimental import pallas as pl
from jax.experimental.pallas import tpu as pltpu
from jax.sharding import PartitionSpec as P


RADIUS = 4
LEVELS = 2
EARLY = 0
LATE = 1
SIDE = 2 * RADIUS
SPAN = 4 * RADIUS
WIN = 2 * RADIUS + 1
WINDOW = WIN * WIN
QUERIES = SIDE * SIDE
SLOTS = 2
LANES = SLOTS * QUERIES
PART_ROWS = 88
EARLY_ROWS = 80
REPLY_ROWS = EARLY_ROWS + PART_ROWS
PEERS_A_STEP = 32
BENCHES = 8
FULL = 32767.0
AXES = ("rows", "cols")


def swapped(upward, downward, axis):
    count = lax.axis_size(axis)
    forward = [(i, i + 1) for i in range(count - 1)]
    backward = [(target, source) for source, target in forward]
    return lax.ppermute(upward, axis, forward), lax.ppermute(downward, axis, backward)


def neighbours(block, axis, dim, width):
    tail = lax.slice_in_dim(block, block.shape[dim] - width, None, axis=dim)
    return swapped(tail, lax.slice_in_dim(block, 0, width, axis=dim), axis)


def pool_level(level_map):
    frame_count, rows_in, cols_in, channels = level_map.shape
    pooled = level_map.astype(jnp.float32).reshape(
        frame_count, rows_in // 2, 2, cols_in // 2, 2, channels
    )
    return jnp.mean(pooled, axis=(2, 4)).astype(jnp.bfloat16)


def window_strips(padded):
    frames, rows, cols, channels = padded.shape
    across = (cols - SIDE) // SIDE
    strips = [
        lax.slice_in_dim(padded, t * SIDE, t * SIDE + SPAN, axis=2) for t in range(across)
    ]
    return jnp.stack(strips).reshape(across * frames * rows, SPAN, channels)


def tile_copy(fmap, send, sems, per_frame, across, band_rows):
    def copy(k, slot):
        frame = k // per_frame
        rest = k % per_frame
        row = frame * band_rows + rest // across * SIDE
        return pltpu.make_async_copy(
            fmap.at[pl.ds(row, SIDE), rest % across],
            send.at[slot // SLOTS, pl.ds(slot % SLOTS * SIDE, SIDE)],
            sems.at[k],
        )

    return copy


def first_body(peers, blocks, tiles_of, per_frame, across, band_rows):
    def kernel(owner, tile, fmap, send, slots, count, labels, notes, sems, note_sem):
        copy = tile_copy(fmap, send, sems, per_frame, across, band_rows)

        def clear(i, carry):
            count[i] = 0
            return carry

        lax.fori_loop(0, LEVELS * peers, clear, 0, unroll=32)

        def blank(i, carry):
            labels[i] = 0
            return carry

        lax.fori_loop(0, LEVELS * SLOTS * peers, blank, 0, unroll=32)

        def place(k, carry):
            for level in (EARLY, LATE):
                own = owner[level, 0, k]
                seen = count[level * peers + own]
                count[level * peers + own] = seen + 1
                slot = own * SLOTS + seen
                slots[level * blocks + k] = slot
                labels[level * SLOTS * peers + slot] = k // per_frame * tiles_of[level] + lax.rem(
                    tile[level, k], tiles_of[level]
                )
                if level == EARLY:
                    copy(k, slot).start()
            return carry

        lax.fori_loop(0, blocks, place, 0, unroll=4)

        lane = lax.broadcasted_iota(jnp.int32, notes.shape[1:], 1)

        def note(peer, carry):
            values = jnp.zeros(notes.shape[1:], jnp.int32)
            for level in range(LEVELS):
                for seen in range(SLOTS):
                    label = labels[(level * peers + peer) * SLOTS + seen]
                    values = jnp.where(lane == level * SLOTS + seen, label, values)
            notes[peer] = values.astype(jnp.float32).astype(jnp.bfloat16)
            return carry

        lax.fori_loop(0, peers, note, 0, unroll=8)
        noted = pltpu.make_async_copy(notes, send.at[:, SLOTS * SIDE], note_sem)
        noted.start()

        def finish(k, carry):
            copy(k, slots[EARLY * blocks + k]).wait()
            return carry

        lax.fori_loop(0, blocks, finish, 0, unroll=8)
        noted.wait()

    return kernel


def second_body(blocks, per_frame, across, band_rows):
    def kernel(slots, fmap, send, sems):
        copy = tile_copy(fmap, send, sems, per_frame, across, band_rows)

        def place(k, carry):
            copy(k, slots[LATE * blocks + k]).start()
            return carry

        def finish(k, carry):
            copy(k, slots[LATE * blocks + k]).wait()
            return carry

        lax.fori_loop(0, blocks, place, 0, unroll=4)
        lax.fori_loop(0, blocks, finish, 0, unroll=8)

    return kernel


def window_table(query, cells, first, i_part, j_part):
    tables = [
        lax.dot_general(
            window.reshape(SPAN * SPAN, -1),
            query,
            (((1,), (1,)), ((), ())),
            preferred_element_type=jnp.float32,
        )
        for window in cells
    ]
    table = jnp.where(first, tables[0], tables[1]).reshape(SPAN, SPAN, LANES)
    for bit in (4, 2, 1):
        left = table.shape[0] - bit
        table = jnp.where(i_part & bit != 0, table[bit:], table[:left])
    table = table.reshape(WIN * SPAN, LANES)
    for bit in (4, 2, 1):
        table = jnp.where(j_part & bit != 0, pltpu.roll(table, WIN * SPAN - bit, 0), table)
    return table


def serve_body(rows, across, tiles, frames, label_of):
    def run(step, queries, strips, flat, store):
        lane = lax.broadcasted_iota(jnp.int32, (1, LANES), 1)
        first = lane < QUERIES
        i_part = lane % QUERIES // SIDE
        j_part = lane % SIDE
        row_id = lax.broadcasted_iota(jnp.int32, (PART_ROWS, LANES), 0)

        def start_of(label):
            tile = label % tiles
            column = tile % across
            return (column * frames + label // tiles) * rows + tile // across * SIDE

        def one(peer, bench):
            cells = [
                strips[pl.ds(start_of(label_of(step * PEERS_A_STEP + peer, slot)), SPAN)]
                for slot in range(SLOTS)
            ]
            table = window_table(queries[peer], cells, first, i_part, j_part)
            for a in range(WIN):
                flat[bench, a * WIN : (a + 1) * WIN, :] = table[a * SPAN : a * SPAN + WIN]
            values = flat[bench]
            top = jnp.max(jnp.abs(values), axis=0, keepdims=True)
            power = jnp.ceil(jnp.log2(jnp.maximum(top, 1e-30)))
            coded = jnp.round(values * (jnp.exp2(-power) * FULL))
            coded = jnp.clip(coded, -FULL, FULL)
            store(peer, row_id, jnp.where(row_id == WINDOW, power, coded).astype(jnp.int32))

        def turn(i, carry):
            for bench in range(BENCHES):
                one(i * BENCHES + bench, bench)
            return carry

        lax.fori_loop(0, PEERS_A_STEP // BENCHES, turn, 0)

    return run


def early_body(rows, across, tiles, frames, peers):
    def kernel(notes, queries, strips, part, others, flat, lines, labels, sem):
        step = pl.program_id(0)

        @pl.when(step == 0)
        def _():
            flat[...] = jnp.zeros_like(flat)

            def line(peer, carry):
                values = notes[peer].astype(jnp.float32).astype(jnp.int32)
                lines[pl.ds(peer, 1), :] = values[:1, : lines.shape[1]]
                return carry

            lax.fori_loop(0, peers, line, 0, unroll=8)
            taken = pltpu.make_async_copy(lines, labels, sem)
            taken.start()
            taken.wait()

            def other(peer, carry):
                for slot in range(SLOTS):
                    others[peer * SLOTS + slot] = labels[peer, LATE * SLOTS + slot]
                return carry

            lax.fori_loop(0, peers, other, 0, unroll=4)

        def store(peer, row_id, coded):
            part[peer] = coded.astype(jnp.int16)

        run = serve_body(rows, across, tiles, frames, lambda p, slot: labels[p, EARLY * SLOTS + slot])
        run(step, queries, strips, flat, store)

    return kernel


def late_body(rows, across, tiles, frames):
    def kernel(labels, queries, strips, part, reply, flat):
        step = pl.program_id(0)

        @pl.when(step == 0)
        def _():
            flat[...] = jnp.zeros_like(flat)

        def store(peer, row_id, coded):
            rest = part[peer, EARLY_ROWS:PART_ROWS].astype(jnp.int32)
            coded = jnp.where(row_id == WINDOW + 1, rest[0:1], coded)
            coded = jnp.where(row_id == WINDOW + 2, rest[1:2], coded)
            reply[peer, :EARLY_ROWS] = part[peer, :EARLY_ROWS]
            reply[peer, EARLY_ROWS:] = coded.astype(jnp.int16)

        run = serve_body(rows, across, tiles, frames, lambda p, slot: labels[p * SLOTS + slot])
        run(step, queries, strips, flat, store)

    return kernel


def finish_body(blocks, groups, scale):
    def kernel(slots, reply, out):
        step = pl.program_id(0)
        low = lax.broadcasted_iota(jnp.int32, (1, LANES), 1) < QUERIES

        def joined(slot, begin, end):
            block = [reply[at // SLOTS, begin:end].astype(jnp.int32) for at in slot]
            straight = jnp.where(low, block[0], block[1])
            turned = pltpu.roll(jnp.where(low, block[1], block[0]), QUERIES, 1)
            kept = [slot[side] % SLOTS == side for side in range(2)]
            left = jnp.where(kept[0], straight, turned)
            right = jnp.where(kept[1], straight, turned)
            return jnp.where(low, left, right).astype(jnp.float32)

        def unit(power):
            return jnp.exp2(power) * (scale / FULL)

        for group in range(groups):
            k = (step * groups + group) * 2
            lanes = slice(group * LANES, (group + 1) * LANES)
            slot = [slots[LATE * blocks + k + side] for side in range(2)]
            late = joined(slot, EARLY_ROWS, REPLY_ROWS)
            out[:, LATE, lanes] = late[:WINDOW] * unit(late[WINDOW : WINDOW + 1])
            slot = [slots[EARLY * blocks + k + side] for side in range(2)]
            early = joined(slot, 0, EARLY_ROWS)
            last = joined(slot, REPLY_ROWS - 8, REPLY_ROWS)
            at = WINDOW - EARLY_ROWS
            factor = unit(last[at + 2 : at + 3])
            out[:EARLY_ROWS, EARLY, lanes] = early * factor
            out[EARLY_ROWS:, EARLY, lanes] = last[at + 1 : at + 2] * factor

    return kernel


def steps(fmap1, fmap2, target_owner, target_tile):
    frames, band_rows, band_cols, channels = fmap1.shape
    peers = lax.axis_size("rows") * lax.axis_size("cols")
    across = band_cols // SIDE
    per_frame = band_rows // SIDE * across
    blocks = frames * per_frame
    across_of = [(band_cols >> l) // SIDE for l in range(LEVELS)]
    tiles_of = [((band_rows >> l) // SIDE) * across_of[l] for l in range(LEVELS)]

    smem = pl.BlockSpec(memory_space=pltpu.SMEM)
    vmem = pl.BlockSpec(memory_space=pltpu.VMEM)
    hbm = pl.BlockSpec(memory_space=pl.ANY)
    tiles = fmap1.reshape(frames * band_rows, across, SIDE, channels)

    def send_shape(parts):
        return jax.ShapeDtypeStruct((peers, parts, SIDE, channels), jnp.bfloat16)

    send_a, slots = pl.pallas_call(
        first_body(peers, blocks, tiles_of, per_frame, across, band_rows),
        in_specs=[smem, smem, vmem],
        out_specs=[hbm, smem],
        out_shape=[
            send_shape(SLOTS * SIDE + 1),
            jax.ShapeDtypeStruct((LEVELS * blocks,), jnp.int32),
        ],
        scratch_shapes=[
            pltpu.SMEM((LEVELS * peers,), jnp.int32),
            pltpu.SMEM((LEVELS * SLOTS * peers,), jnp.int32),
            pltpu.VMEM((peers, SIDE, channels), jnp.bfloat16),
            pltpu.SemaphoreType.DMA((blocks,)),
            pltpu.SemaphoreType.DMA,
        ],
        name="build_a",
    )(target_owner.transpose(0, 2, 1), target_tile, tiles)
    send_b = pl.pallas_call(
        second_body(blocks, per_frame, across, band_rows),
        in_specs=[smem, vmem],
        out_specs=hbm,
        out_shape=send_shape(SLOTS * SIDE),
        scratch_shapes=[pltpu.SemaphoreType.DMA((blocks,))],
        name="build_b",
    )(slots, tiles)

    def exchange(value):
        return lax.all_to_all(value, AXES, split_axis=0, concat_axis=0, tiled=True)

    arrived = [exchange(send.reshape(peers, -1, channels)) for send in (send_a, send_b)]

    low, high = neighbours(fmap2, "rows", 1, SIDE)
    edges = [
        jnp.concatenate([lax.slice_in_dim(part, *span, axis=2) for part in (low, fmap2, high)], axis=1)
        for span in ((0, SIDE), (band_cols - SIDE, band_cols))
    ]
    west, east = swapped(edges[1], edges[0], "cols")
    tall = jnp.concatenate([low, fmap2, high], axis=1)
    wide = jnp.concatenate([west, tall, east], axis=2)
    maps = [wide[:, RADIUS:-RADIUS, RADIUS:-RADIUS], pool_level(wide)]

    strips = []
    for level in range(LEVELS):
        strips.append(window_strips(maps[level]))

    def facts(level):
        return maps[level].shape[1], across_of[level], tiles_of[level], frames

    grid = (peers // PEERS_A_STEP,)
    query_block = pl.BlockSpec((PEERS_A_STEP, LANES, channels), lambda s, *_: (s, 0, 0))
    part_block = pl.BlockSpec((PEERS_A_STEP, PART_ROWS, LANES), lambda s, *_: (s, 0, 0))
    flat = pltpu.VMEM((BENCHES, PART_ROWS, LANES), jnp.float32)

    def strip_block(level):
        return pl.BlockSpec(strips[level].shape, lambda s, *_: (0, 0, 0))

    part, labels = pl.pallas_call(
        early_body(*facts(EARLY), peers),
        grid=grid,
        in_specs=[
            pl.BlockSpec((peers, SIDE, channels), lambda s: (0, LANES // SIDE, 0)),
            query_block,
            strip_block(EARLY),
        ],
        out_specs=[part_block, smem],
        out_shape=[
            jax.ShapeDtypeStruct((peers, PART_ROWS, LANES), jnp.int16),
            jax.ShapeDtypeStruct((peers * SLOTS,), jnp.int32),
        ],
        scratch_shapes=[
            flat,
            pltpu.VMEM((peers, 128), jnp.int32),
            pltpu.SMEM((peers, 128), jnp.int32),
            pltpu.SemaphoreType.DMA,
        ],
        name="serve_a",
    )(arrived[0], arrived[0], strips[EARLY])
    served = pl.pallas_call(
        late_body(*facts(LATE)),
        grid_spec=pltpu.PrefetchScalarGridSpec(
            num_scalar_prefetch=1,
            grid=grid,
            in_specs=[query_block, strip_block(LATE), part_block],
            out_specs=pl.BlockSpec(
                (PEERS_A_STEP, REPLY_ROWS, LANES), lambda s, *_: (s, 0, 0)
            ),
            scratch_shapes=[flat],
        ),
        out_shape=jax.ShapeDtypeStruct((peers, REPLY_ROWS, LANES), jnp.int16),
        name="serve_b",
    )(labels, arrived[1], strips[LATE], part)
    reply = exchange(served)

    groups = 8
    width = groups * LANES
    whole = pl.BlockSpec((peers, REPLY_ROWS, LANES), lambda s, _: (0, 0, 0))
    out = pl.pallas_call(
        finish_body(blocks, groups, channels ** (-0.5)),
        grid_spec=pltpu.PrefetchScalarGridSpec(
            num_scalar_prefetch=1,
            grid=(blocks * QUERIES // width,),
            in_specs=[whole],
            out_specs=pl.BlockSpec((WINDOW, LEVELS, width), lambda s, _: (0, 0, s)),
        ),
        out_shape=jax.ShapeDtypeStruct((WINDOW, LEVELS, blocks * QUERIES), jnp.float32),
        name="finish",
    )(slots, reply)
    return out.transpose(1, 0, 2)


def solution(mesh):
    in_specs = (
        P(None, "rows", "cols", None),
        P(None, "rows", "cols", None),
        P(None, AXES, None),
        P(None, AXES),
    )
    out_specs = P(None, None, AXES)
    return jax.shard_map(steps, mesh=mesh, in_specs=in_specs, out_specs=out_specs, check_vma=False)
```

```python
import jax
import jax.numpy as jnp
from jax import lax
from jax.experimental import pallas as pl
from jax.experimental.pallas import tpu as pltpu
from jax.sharding import PartitionSpec as P


RADIUS = 4
LEVELS = 2
EARLY = 0
LATE = 1
SIDE = 2 * RADIUS
SPAN = 4 * RADIUS
WIN = 2 * RADIUS + 1
WINDOW = WIN * WIN
QUERIES = SIDE * SIDE
SLOTS = 2
LANES = SLOTS * QUERIES
PART_ROWS = 88
EARLY_ROWS = 80
REPLY_ROWS = EARLY_ROWS + PART_ROWS
PEERS_A_STEP = 32
BENCHES = 8
FULL = 32767.0
MIB = 1 << 20
SERVE_B_VMEM = 14 * MIB
FINISH_VMEM = 12 * MIB
AXES = ("rows", "cols")


def swapped(upward, downward, axis):
    count = lax.axis_size(axis)
    forward = [(i, i + 1) for i in range(count - 1)]
    backward = [(target, source) for source, target in forward]
    return lax.ppermute(upward, axis, forward), lax.ppermute(downward, axis, backward)


def neighbours(block, axis, dim, width):
    tail = lax.slice_in_dim(block, block.shape[dim] - width, None, axis=dim)
    return swapped(tail, lax.slice_in_dim(block, 0, width, axis=dim), axis)


def pool_level(level_map):
    frame_count, rows_in, cols_in, channels = level_map.shape
    pooled = level_map.astype(jnp.float32).reshape(
        frame_count, rows_in // 2, 2, cols_in // 2, 2, channels
    )
    return jnp.mean(pooled, axis=(2, 4)).astype(jnp.bfloat16)


def window_strips(padded):
    frames, rows, cols, channels = padded.shape
    across = (cols - SIDE) // SIDE
    strips = [
        lax.slice_in_dim(padded, t * SIDE, t * SIDE + SPAN, axis=2) for t in range(across)
    ]
    return jnp.stack(strips).reshape(across * frames * rows, SPAN, channels)


def tile_copy(fmap, send, sems, per_frame, across, band_rows):
    def copy(k, slot):
        frame = k // per_frame
        rest = k % per_frame
        row = frame * band_rows + rest // across * SIDE
        return pltpu.make_async_copy(
            fmap.at[pl.ds(row, SIDE), rest % across],
            send.at[slot // SLOTS, pl.ds(slot % SLOTS * SIDE, SIDE)],
            sems.at[k],
        )

    return copy


def first_body(peers, blocks, tiles_of, per_frame, across, band_rows):
    def kernel(owner, tile, fmap, send, slots, count, labels, notes, sems, note_sem):
        copy = tile_copy(fmap, send, sems, per_frame, across, band_rows)

        def clear(i, carry):
            count[i] = 0
            return carry

        lax.fori_loop(0, LEVELS * peers, clear, 0, unroll=32)

        def blank(i, carry):
            labels[i] = 0
            return carry

        lax.fori_loop(0, LEVELS * SLOTS * peers, blank, 0, unroll=32)

        def place(k, carry):
            for level in (EARLY, LATE):
                own = owner[level, 0, k]
                seen = count[level * peers + own]
                count[level * peers + own] = seen + 1
                slot = own * SLOTS + seen
                slots[level * blocks + k] = slot
                labels[level * SLOTS * peers + slot] = k // per_frame * tiles_of[level] + lax.rem(
                    tile[level, k], tiles_of[level]
                )
                if level == EARLY:
                    copy(k, slot).start()
            return carry

        lax.fori_loop(0, blocks, place, 0, unroll=4)

        lane = lax.broadcasted_iota(jnp.int32, notes.shape[1:], 1)

        def note(peer, carry):
            values = jnp.zeros(notes.shape[1:], jnp.int32)
            for level in range(LEVELS):
                for seen in range(SLOTS):
                    label = labels[(level * peers + peer) * SLOTS + seen]
                    values = jnp.where(lane == level * SLOTS + seen, label, values)
            notes[peer] = values.astype(jnp.float32).astype(jnp.bfloat16)
            return carry

        lax.fori_loop(0, peers, note, 0, unroll=8)
        noted = pltpu.make_async_copy(notes, send.at[:, SLOTS * SIDE], note_sem)
        noted.start()

        def finish(k, carry):
            copy(k, slots[EARLY * blocks + k]).wait()
            return carry

        lax.fori_loop(0, blocks, finish, 0, unroll=8)
        noted.wait()

    return kernel


def second_body(blocks, per_frame, across, band_rows):
    def kernel(slots, fmap, send, sems):
        copy = tile_copy(fmap, send, sems, per_frame, across, band_rows)

        def place(k, carry):
            copy(k, slots[LATE * blocks + k]).start()
            return carry

        def finish(k, carry):
            copy(k, slots[LATE * blocks + k]).wait()
            return carry

        lax.fori_loop(0, blocks, place, 0, unroll=4)
        lax.fori_loop(0, blocks, finish, 0, unroll=8)

    return kernel


def window_table(query, cells, first, i_part, j_part):
    tables = [
        lax.dot_general(
            window.reshape(SPAN * SPAN, -1),
            query,
            (((1,), (1,)), ((), ())),
            preferred_element_type=jnp.float32,
        )
        for window in cells
    ]
    table = jnp.where(first, tables[0], tables[1]).reshape(SPAN, SPAN, LANES)
    for bit in (4, 2, 1):
        left = table.shape[0] - bit
        table = jnp.where(i_part & bit != 0, table[bit:], table[:left])
    table = table.reshape(WIN * SPAN, LANES)
    for bit in (4, 2, 1):
        table = jnp.where(j_part & bit != 0, pltpu.roll(table, WIN * SPAN - bit, 0), table)
    return table


def serve_body(rows, across, tiles, frames, label_of):
    def run(step, queries, strips, flat, store):
        lane = lax.broadcasted_iota(jnp.int32, (1, LANES), 1)
        first = lane < QUERIES
        i_part = lane % QUERIES // SIDE
        j_part = lane % SIDE
        row_id = lax.broadcasted_iota(jnp.int32, (PART_ROWS, LANES), 0)

        def start_of(label):
            tile = label % tiles
            column = tile % across
            return (column * frames + label // tiles) * rows + tile // across * SIDE

        def one(peer, bench):
            cells = [
                strips[pl.ds(start_of(label_of(step * PEERS_A_STEP + peer, slot)), SPAN)]
                for slot in range(SLOTS)
            ]
            table = window_table(queries[peer], cells, first, i_part, j_part)
            for a in range(WIN):
                flat[bench, a * WIN : (a + 1) * WIN, :] = table[a * SPAN : a * SPAN + WIN]
            values = flat[bench]
            top = jnp.max(jnp.abs(values), axis=0, keepdims=True)
            power = jnp.ceil(jnp.log2(jnp.maximum(top, 1e-30)))
            coded = jnp.round(values * (jnp.exp2(-power) * FULL))
            coded = jnp.clip(coded, -FULL, FULL)
            store(peer, row_id, jnp.where(row_id == WINDOW, power, coded).astype(jnp.int32))

        def turn(i, carry):
            for bench in range(BENCHES):
                one(i * BENCHES + bench, bench)
            return carry

        lax.fori_loop(0, PEERS_A_STEP // BENCHES, turn, 0)

    return run


def early_body(rows, across, tiles, frames, peers):
    def kernel(notes, queries, strips, part, others, flat, lines, labels, sem):
        step = pl.program_id(0)

        @pl.when(step == 0)
        def _():
            flat[...] = jnp.zeros_like(flat)

            def line(peer, carry):
                values = notes[peer].astype(jnp.float32).astype(jnp.int32)
                lines[pl.ds(peer, 1), :] = values[:1, : lines.shape[1]]
                return carry

            lax.fori_loop(0, peers, line, 0, unroll=8)
            taken = pltpu.make_async_copy(lines, labels, sem)
            taken.start()
            taken.wait()

            def other(peer, carry):
                for slot in range(SLOTS):
                    others[peer * SLOTS + slot] = labels[peer, LATE * SLOTS + slot]
                return carry

            lax.fori_loop(0, peers, other, 0, unroll=4)

        def store(peer, row_id, coded):
            part[peer] = coded.astype(jnp.int16)

        run = serve_body(rows, across, tiles, frames, lambda p, slot: labels[p, EARLY * SLOTS + slot])
        run(step, queries, strips, flat, store)

    return kernel


def late_body(rows, across, tiles, frames):
    def kernel(labels, queries, strips, part, reply, flat):
        step = pl.program_id(0)

        @pl.when(step == 0)
        def _():
            flat[...] = jnp.zeros_like(flat)

        def store(peer, row_id, coded):
            rest = part[peer, EARLY_ROWS:PART_ROWS].astype(jnp.int32)
            coded = jnp.where(row_id == WINDOW + 1, rest[0:1], coded)
            coded = jnp.where(row_id == WINDOW + 2, rest[1:2], coded)
            reply[peer, :EARLY_ROWS] = part[peer, :EARLY_ROWS]
            reply[peer, EARLY_ROWS:] = coded.astype(jnp.int16)

        run = serve_body(rows, across, tiles, frames, lambda p, slot: labels[p * SLOTS + slot])
        run(step, queries, strips, flat, store)

    return kernel


def finish_body(blocks, groups, scale):
    def kernel(slots, reply, out):
        step = pl.program_id(0)
        low = lax.broadcasted_iota(jnp.int32, (1, LANES), 1) < QUERIES

        def joined(slot, begin, end):
            block = [reply[at // SLOTS, begin:end].astype(jnp.int32) for at in slot]
            straight = jnp.where(low, block[0], block[1])
            turned = pltpu.roll(jnp.where(low, block[1], block[0]), QUERIES, 1)
            kept = [slot[side] % SLOTS == side for side in range(2)]
            left = jnp.where(kept[0], straight, turned)
            right = jnp.where(kept[1], straight, turned)
            return jnp.where(low, left, right).astype(jnp.float32)

        def unit(power):
            return jnp.exp2(power) * (scale / FULL)

        for group in range(groups):
            k = (step * groups + group) * 2
            lanes = slice(group * LANES, (group + 1) * LANES)
            slot = [slots[LATE * blocks + k + side] for side in range(2)]
            late = joined(slot, EARLY_ROWS, REPLY_ROWS)
            out[:, LATE, lanes] = late[:WINDOW] * unit(late[WINDOW : WINDOW + 1])
            slot = [slots[EARLY * blocks + k + side] for side in range(2)]
            early = joined(slot, 0, EARLY_ROWS)
            last = joined(slot, REPLY_ROWS - 8, REPLY_ROWS)
            at = WINDOW - EARLY_ROWS
            factor = unit(last[at + 2 : at + 3])
            out[:EARLY_ROWS, EARLY, lanes] = early * factor
            out[EARLY_ROWS:, EARLY, lanes] = last[at + 1 : at + 2] * factor

    return kernel


def steps(fmap1, fmap2, target_owner, target_tile):
    frames, band_rows, band_cols, channels = fmap1.shape
    peers = lax.axis_size("rows") * lax.axis_size("cols")
    across = band_cols // SIDE
    per_frame = band_rows // SIDE * across
    blocks = frames * per_frame
    across_of = [(band_cols >> l) // SIDE for l in range(LEVELS)]
    tiles_of = [((band_rows >> l) // SIDE) * across_of[l] for l in range(LEVELS)]

    smem = pl.BlockSpec(memory_space=pltpu.SMEM)
    vmem = pl.BlockSpec(memory_space=pltpu.VMEM)
    hbm = pl.BlockSpec(memory_space=pl.ANY)
    tiles = fmap1.reshape(frames * band_rows, across, SIDE, channels)

    def send_shape(parts):
        return jax.ShapeDtypeStruct((peers, parts, SIDE, channels), jnp.bfloat16)

    send_a, slots = pl.pallas_call(
        first_body(peers, blocks, tiles_of, per_frame, across, band_rows),
        in_specs=[smem, smem, vmem],
        out_specs=[hbm, smem],
        out_shape=[
            send_shape(SLOTS * SIDE + 1),
            jax.ShapeDtypeStruct((LEVELS * blocks,), jnp.int32),
        ],
        scratch_shapes=[
            pltpu.SMEM((LEVELS * peers,), jnp.int32),
            pltpu.SMEM((LEVELS * SLOTS * peers,), jnp.int32),
            pltpu.VMEM((peers, SIDE, channels), jnp.bfloat16),
            pltpu.SemaphoreType.DMA((blocks,)),
            pltpu.SemaphoreType.DMA,
        ],
        name="build_a",
    )(target_owner.transpose(0, 2, 1), target_tile, tiles)
    send_b = pl.pallas_call(
        second_body(blocks, per_frame, across, band_rows),
        in_specs=[smem, vmem],
        out_specs=hbm,
        out_shape=send_shape(SLOTS * SIDE),
        scratch_shapes=[pltpu.SemaphoreType.DMA((blocks,))],
        name="build_b",
    )(slots, tiles)

    def exchange(value):
        return lax.all_to_all(value, AXES, split_axis=0, concat_axis=0, tiled=True)

    arrived = [exchange(send.reshape(peers, -1, channels)) for send in (send_a, send_b)]

    low, high = neighbours(fmap2, "rows", 1, SIDE)
    edges = [
        jnp.concatenate([lax.slice_in_dim(part, *span, axis=2) for part in (low, fmap2, high)], axis=1)
        for span in ((0, SIDE), (band_cols - SIDE, band_cols))
    ]
    west, east = swapped(edges[1], edges[0], "cols")
    tall = jnp.concatenate([low, fmap2, high], axis=1)
    wide = jnp.concatenate([west, tall, east], axis=2)
    maps = [wide[:, RADIUS:-RADIUS, RADIUS:-RADIUS], pool_level(wide)]

    strips = []
    for level in range(LEVELS):
        strips.append(window_strips(maps[level]))

    def facts(level):
        return maps[level].shape[1], across_of[level], tiles_of[level], frames

    grid = (peers // PEERS_A_STEP,)
    query_block = pl.BlockSpec((PEERS_A_STEP, LANES, channels), lambda s, *_: (s, 0, 0))
    part_block = pl.BlockSpec((PEERS_A_STEP, PART_ROWS, LANES), lambda s, *_: (s, 0, 0))
    flat = pltpu.VMEM((BENCHES, PART_ROWS, LANES), jnp.float32)

    def strip_block(level):
        return pl.BlockSpec(strips[level].shape, lambda s, *_: (0, 0, 0))

    part, labels = pl.pallas_call(
        early_body(*facts(EARLY), peers),
        grid=grid,
        in_specs=[
            pl.BlockSpec((peers, SIDE, channels), lambda s: (0, LANES // SIDE, 0)),
            query_block,
            strip_block(EARLY),
        ],
        out_specs=[part_block, smem],
        out_shape=[
            jax.ShapeDtypeStruct((peers, PART_ROWS, LANES), jnp.int16),
            jax.ShapeDtypeStruct((peers * SLOTS,), jnp.int32),
        ],
        scratch_shapes=[
            flat,
            pltpu.VMEM((peers, 128), jnp.int32),
            pltpu.SMEM((peers, 128), jnp.int32),
            pltpu.SemaphoreType.DMA,
        ],
        name="serve_a",
    )(arrived[0], arrived[0], strips[EARLY])
    served = pl.pallas_call(
        late_body(*facts(LATE)),
        grid_spec=pltpu.PrefetchScalarGridSpec(
            num_scalar_prefetch=1,
            grid=grid,
            in_specs=[query_block, strip_block(LATE), part_block],
            out_specs=pl.BlockSpec(
                (PEERS_A_STEP, REPLY_ROWS, LANES), lambda s, *_: (s, 0, 0)
            ),
            scratch_shapes=[flat],
        ),
        out_shape=jax.ShapeDtypeStruct((peers, REPLY_ROWS, LANES), jnp.int16),
        compiler_params=pltpu.CompilerParams(vmem_limit_bytes=SERVE_B_VMEM),
        name="serve_b",
    )(labels, arrived[1], strips[LATE], part)
    reply = exchange(served)

    groups = 8
    width = groups * LANES
    whole = pl.BlockSpec((peers, REPLY_ROWS, LANES), lambda s, _: (0, 0, 0))
    out = pl.pallas_call(
        finish_body(blocks, groups, channels ** (-0.5)),
        grid_spec=pltpu.PrefetchScalarGridSpec(
            num_scalar_prefetch=1,
            grid=(blocks * QUERIES // width,),
            in_specs=[whole],
            out_specs=pl.BlockSpec((WINDOW, LEVELS, width), lambda s, _: (0, 0, s)),
        ),
        out_shape=jax.ShapeDtypeStruct((WINDOW, LEVELS, blocks * QUERIES), jnp.float32),
        compiler_params=pltpu.CompilerParams(vmem_limit_bytes=FINISH_VMEM),
        name="finish",
    )(slots, reply)
    return out.transpose(1, 0, 2)


def solution(mesh):
    in_specs = (
        P(None, "rows", "cols", None),
        P(None, "rows", "cols", None),
        P(None, AXES, None),
        P(None, AXES),
    )
    out_specs = P(None, None, AXES)
    return jax.shard_map(steps, mesh=mesh, in_specs=in_specs, out_specs=out_specs, check_vma=False)
```

```python
import jax
import jax.numpy as jnp
from jax import lax
from jax.experimental import pallas as pl
from jax.experimental.pallas import tpu as pltpu
from jax.sharding import PartitionSpec as P


RADIUS = 4
LEVELS = 2
SIDE = 2 * RADIUS
SPAN = 4 * RADIUS
WIN = 2 * RADIUS + 1
WINDOW = WIN * WIN
QUERIES = SIDE * SIDE
SLOTS = 2
LANES = SLOTS * QUERIES
REPLY_ROWS = -(-(WINDOW + 1) // 8) * 8
PEERS_A_STEP = 16
BENCHES = 8
FULL = 32767.0
FINISH_VMEM = 16 << 20
AXES = ("rows", "cols")


def swapped(upward, downward, axis):
    count = lax.axis_size(axis)
    forward = [(i, i + 1) for i in range(count - 1)]
    backward = [(target, source) for source, target in forward]
    return lax.ppermute(upward, axis, forward), lax.ppermute(downward, axis, backward)


def neighbours(block, axis, dim, width):
    tail = lax.slice_in_dim(block, block.shape[dim] - width, None, axis=dim)
    return swapped(tail, lax.slice_in_dim(block, 0, width, axis=dim), axis)


def pool_level(level_map):
    frame_count, rows_in, cols_in, channels = level_map.shape
    pooled = level_map.astype(jnp.float32).reshape(
        frame_count, rows_in // 2, 2, cols_in // 2, 2, channels
    )
    return jnp.mean(pooled, axis=(2, 4)).astype(jnp.bfloat16)


def window_strips(padded):
    frames, rows, cols, channels = padded.shape
    across = (cols - SIDE) // SIDE
    strips = [
        lax.slice_in_dim(padded, t * SIDE, t * SIDE + SPAN, axis=2) for t in range(across)
    ]
    return jnp.stack(strips).reshape(across * frames * rows, SPAN, channels)


def tile_copy(fmap, send, sems, per_frame, across, band_rows):
    def copy(k, slot):
        frame = k // per_frame
        rest = k % per_frame
        row = frame * band_rows + rest // across * SIDE
        return pltpu.make_async_copy(
            fmap.at[pl.ds(row, SIDE), rest % across],
            send.at[slot // SLOTS, pl.ds(slot % SLOTS * SIDE, SIDE)],
            sems.at[k],
        )

    return copy


def first_body(peers, blocks, tiles_of, per_frame, across, band_rows):
    last = LEVELS - 1

    def kernel(owner, tile, fmap, send, slots, count, labels, notes, sems, note_sem):
        copy = tile_copy(fmap, send, sems, per_frame, across, band_rows)

        def clear(i, carry):
            count[i] = 0
            return carry

        lax.fori_loop(0, LEVELS * peers, clear, 0, unroll=32)

        def blank(i, carry):
            labels[i] = 0
            return carry

        lax.fori_loop(0, LEVELS * SLOTS * peers, blank, 0, unroll=32)

        def place(k, carry):
            for level in reversed(range(LEVELS)):
                own = owner[level, 0, k]
                seen = count[level * peers + own]
                count[level * peers + own] = seen + 1
                slot = own * SLOTS + seen
                slots[level * blocks + k] = slot
                labels[level * SLOTS * peers + slot] = k // per_frame * tiles_of[level] + lax.rem(
                    tile[level, k], tiles_of[level]
                )
                if level == last:
                    copy(k, slot).start()
            return carry

        lax.fori_loop(0, blocks, place, 0, unroll=4)

        lane = lax.broadcasted_iota(jnp.int32, notes.shape[1:], 1)

        def note(peer, carry):
            values = jnp.zeros(notes.shape[1:], jnp.int32)
            for level in range(LEVELS):
                for seen in range(SLOTS):
                    label = labels[(level * peers + peer) * SLOTS + seen]
                    values = jnp.where(lane == level * SLOTS + seen, label, values)
            notes[peer] = values.astype(jnp.float32).astype(jnp.bfloat16)
            return carry

        lax.fori_loop(0, peers, note, 0, unroll=8)
        noted = pltpu.make_async_copy(notes, send.at[:, SLOTS * SIDE], note_sem)
        noted.start()

        def finish(k, carry):
            copy(k, slots[last * blocks + k]).wait()
            return carry

        lax.fori_loop(0, blocks, finish, 0, unroll=8)
        noted.wait()

    return kernel


def second_body(blocks, per_frame, across, band_rows):
    def kernel(slots, fmap, send, sems):
        copy = tile_copy(fmap, send, sems, per_frame, across, band_rows)

        def place(k, carry):
            copy(k, slots[k]).start()
            return carry

        def finish(k, carry):
            copy(k, slots[k]).wait()
            return carry

        lax.fori_loop(0, blocks, place, 0, unroll=4)
        lax.fori_loop(0, blocks, finish, 0, unroll=8)

    return kernel


def serve_body(level, rows, across, tiles, frames, peers):
    def kernel(notes, queries, strips, reply, flat, lines, labels, sem):
        step = pl.program_id(0)
        lane = lax.broadcasted_iota(jnp.int32, (1, LANES), 1)
        first = lane < QUERIES
        i_part = lane % QUERIES // SIDE
        j_part = lane % SIDE
        row_id = lax.broadcasted_iota(jnp.int32, (REPLY_ROWS, LANES), 0)

        @pl.when(step == 0)
        def _():
            flat[...] = jnp.zeros_like(flat)

            def line(peer, carry):
                values = notes[peer].astype(jnp.float32).astype(jnp.int32)
                lines[pl.ds(peer, 1), :] = values[:1, : lines.shape[1]]
                return carry

            lax.fori_loop(0, peers, line, 0, unroll=8)
            taken = pltpu.make_async_copy(lines, labels, sem)
            taken.start()
            taken.wait()

        def start_of(label):
            tile = label % tiles
            column = tile % across
            return (column * frames + label // tiles) * rows + tile // across * SIDE

        def one(peer, bench):
            query = queries[peer]
            tables = []
            for slot in range(SLOTS):
                label = labels[step * PEERS_A_STEP + peer, level * SLOTS + slot]
                cells = strips[pl.ds(start_of(label), SPAN)]
                tables.append(
                    lax.dot_general(
                        cells.reshape(SPAN * SPAN, -1),
                        query,
                        (((1,), (1,)), ((), ())),
                        preferred_element_type=jnp.float32,
                    )
                )
            table = jnp.where(first, tables[0], tables[1])
            table = table.reshape(SPAN, SPAN, LANES)
            for bit in (4, 2, 1):
                left = table.shape[0] - bit
                table = jnp.where(i_part & bit != 0, table[bit:], table[:left])
            table = table.reshape(WIN * SPAN, LANES)
            for bit in (4, 2, 1):
                table = jnp.where(
                    j_part & bit != 0, pltpu.roll(table, WIN * SPAN - bit, 0), table
                )
            for a in range(WIN):
                flat[bench, a * WIN : (a + 1) * WIN, :] = table[a * SPAN : a * SPAN + WIN]
            values = flat[bench]
            top = jnp.max(jnp.abs(values), axis=0, keepdims=True)
            power = jnp.ceil(jnp.log2(jnp.maximum(top, 1e-30)))
            coded = jnp.round(values * (jnp.exp2(-power) * FULL))
            coded = jnp.clip(coded, -FULL, FULL)
            coded = jnp.where(row_id == WINDOW, power, coded)
            reply[peer] = coded.astype(jnp.int32).astype(jnp.int16)

        def turn(i, carry):
            for bench in range(BENCHES):
                one(i * BENCHES + bench, bench)
            return carry

        lax.fori_loop(0, PEERS_A_STEP // BENCHES, turn, 0)

    return kernel


def finish_body(blocks, groups, scale):
    def kernel(slots, reply0, reply1, out):
        step = pl.program_id(0)
        low = lax.broadcasted_iota(jnp.int32, (1, LANES), 1) < QUERIES
        for level, reply in enumerate((reply0, reply1)):
            for group in range(groups):
                k = level * blocks + (step * groups + group) * 2
                slot = [slots[k + side] for side in range(2)]
                block = [reply[at // SLOTS].astype(jnp.int32) for at in slot]
                straight = jnp.where(low, block[0], block[1])
                turned = pltpu.roll(jnp.where(low, block[1], block[0]), QUERIES, 1)
                kept = [slot[side] % SLOTS == side for side in range(2)]
                left = jnp.where(kept[0], straight, turned)
                right = jnp.where(kept[1], straight, turned)
                both = jnp.where(low, left, right).astype(jnp.float32)
                factor = jnp.exp2(both[WINDOW : WINDOW + 1]) * (scale / FULL)
                out[:, level, group * LANES : (group + 1) * LANES] = both[:WINDOW] * factor

    return kernel


def steps(fmap1, fmap2, target_owner, target_tile):
    frames, band_rows, band_cols, channels = fmap1.shape
    peers = lax.axis_size("rows") * lax.axis_size("cols")
    across = band_cols // SIDE
    per_frame = band_rows // SIDE * across
    blocks = frames * per_frame
    across_of = [(band_cols >> l) // SIDE for l in range(LEVELS)]
    tiles_of = [((band_rows >> l) // SIDE) * across_of[l] for l in range(LEVELS)]

    smem = pl.BlockSpec(memory_space=pltpu.SMEM)
    vmem = pl.BlockSpec(memory_space=pltpu.VMEM)
    hbm = pl.BlockSpec(memory_space=pl.ANY)
    tiles = fmap1.reshape(frames * band_rows, across, SIDE, channels)

    def send_shape(parts):
        return jax.ShapeDtypeStruct((peers, parts, SIDE, channels), jnp.bfloat16)

    send1, slots = pl.pallas_call(
        first_body(peers, blocks, tiles_of, per_frame, across, band_rows),
        in_specs=[smem, smem, vmem],
        out_specs=[hbm, smem],
        out_shape=[
            send_shape(SLOTS * SIDE + 1),
            jax.ShapeDtypeStruct((LEVELS * blocks,), jnp.int32),
        ],
        scratch_shapes=[
            pltpu.SMEM((LEVELS * peers,), jnp.int32),
            pltpu.SMEM((LEVELS * SLOTS * peers,), jnp.int32),
            pltpu.VMEM((peers, SIDE, channels), jnp.bfloat16),
            pltpu.SemaphoreType.DMA((blocks,)),
            pltpu.SemaphoreType.DMA,
        ],
        name="build1",
    )(target_owner.transpose(0, 2, 1), target_tile, tiles)
    send0 = pl.pallas_call(
        second_body(blocks, per_frame, across, band_rows),
        in_specs=[smem, vmem],
        out_specs=hbm,
        out_shape=send_shape(SLOTS * SIDE),
        scratch_shapes=[pltpu.SemaphoreType.DMA((blocks,))],
        name="build0",
    )(slots, tiles)

    def exchange(value):
        return lax.all_to_all(value, AXES, split_axis=0, concat_axis=0, tiled=True)

    arrived = [exchange(send.reshape(peers, -1, channels)) for send in (send0, send1)]

    low, high = neighbours(fmap2, "rows", 1, SIDE)
    edges = [
        jnp.concatenate([lax.slice_in_dim(part, *span, axis=2) for part in (low, fmap2, high)], axis=1)
        for span in ((0, SIDE), (band_cols - SIDE, band_cols))
    ]
    west, east = swapped(edges[1], edges[0], "cols")
    tall = jnp.concatenate([low, fmap2, high], axis=1)
    wide = jnp.concatenate([west, tall, east], axis=2)
    maps = [wide[:, RADIUS:-RADIUS, RADIUS:-RADIUS], pool_level(wide)]

    replies = []
    for level in range(LEVELS):
        strips = window_strips(maps[level])
        served = pl.pallas_call(
            serve_body(level, maps[level].shape[1], across_of[level], tiles_of[level], frames, peers),
            grid=(peers // PEERS_A_STEP,),
            in_specs=[
                pl.BlockSpec((peers, SIDE, channels), lambda s: (0, LANES // SIDE, 0)),
                pl.BlockSpec((PEERS_A_STEP, LANES, channels), lambda s: (s, 0, 0)),
                pl.BlockSpec(strips.shape, lambda s: (0, 0, 0)),
            ],
            out_specs=pl.BlockSpec((PEERS_A_STEP, REPLY_ROWS, LANES), lambda s: (s, 0, 0)),
            scratch_shapes=[
                pltpu.VMEM((BENCHES, REPLY_ROWS, LANES), jnp.float32),
                pltpu.VMEM((peers, 128), jnp.int32),
                pltpu.SMEM((peers, 128), jnp.int32),
                pltpu.SemaphoreType.DMA,
            ],
            out_shape=jax.ShapeDtypeStruct((peers, REPLY_ROWS, LANES), jnp.int16),
        )(arrived[1], arrived[level], strips)
        replies.append(exchange(served))

    groups = 8
    width = groups * LANES
    whole = pl.BlockSpec((peers, REPLY_ROWS, LANES), lambda s, _: (0, 0, 0))
    out = pl.pallas_call(
        finish_body(blocks, groups, channels ** (-0.5)),
        grid_spec=pltpu.PrefetchScalarGridSpec(
            num_scalar_prefetch=1,
            grid=(blocks * QUERIES // width,),
            in_specs=[whole, whole],
            out_specs=pl.BlockSpec((WINDOW, LEVELS, width), lambda s, _: (0, 0, s)),
        ),
        out_shape=jax.ShapeDtypeStruct((WINDOW, LEVELS, blocks * QUERIES), jnp.float32),
        compiler_params=pltpu.CompilerParams(vmem_limit_bytes=FINISH_VMEM),
        name="finish",
    )(slots, *replies)
    return out.transpose(1, 0, 2)


def solution(mesh):
    in_specs = (
        P(None, "rows", "cols", None),
        P(None, "rows", "cols", None),
        P(None, AXES, None),
        P(None, AXES),
    )
    out_specs = P(None, None, AXES)
    return jax.shard_map(steps, mesh=mesh, in_specs=in_specs, out_specs=out_specs, check_vma=False)
```

```python
import jax
import jax.numpy as jnp
from jax import lax
from jax.experimental import pallas as pl
from jax.experimental.pallas import tpu as pltpu
from jax.sharding import PartitionSpec as P


RADIUS = 4
LEVELS = 2
SIDE = 2 * RADIUS
SPAN = 4 * RADIUS
WIN = 2 * RADIUS + 1
WINDOW = WIN * WIN
QUERIES = SIDE * SIDE
SLOTS = 2
LANES = SLOTS * QUERIES
REPLY_ROWS = -(-(WINDOW + 1) // 8) * 8
PEERS_A_STEP = 16
BENCHES = 8
FULL = 32767.0
FINISH_VMEM = 16 << 20
AXES = ("rows", "cols")


def swapped(upward, downward, axis):
    count = lax.axis_size(axis)
    forward = [(i, i + 1) for i in range(count - 1)]
    backward = [(target, source) for source, target in forward]
    return lax.ppermute(upward, axis, forward), lax.ppermute(downward, axis, backward)


def neighbours(block, axis, dim, width):
    tail = lax.slice_in_dim(block, block.shape[dim] - width, None, axis=dim)
    return swapped(tail, lax.slice_in_dim(block, 0, width, axis=dim), axis)


def pool_level(level_map):
    frame_count, rows_in, cols_in, channels = level_map.shape
    pooled = level_map.astype(jnp.float32).reshape(
        frame_count, rows_in // 2, 2, cols_in // 2, 2, channels
    )
    return jnp.mean(pooled, axis=(2, 4)).astype(jnp.bfloat16)


def window_strips(padded):
    frames, rows, cols, channels = padded.shape
    across = (cols - SIDE) // SIDE
    strips = [
        lax.slice_in_dim(padded, t * SIDE, t * SIDE + SPAN, axis=2) for t in range(across)
    ]
    return jnp.stack(strips).reshape(across * frames * rows, SPAN, channels)


def tile_copy(fmap, send, sems, per_frame, across, band_rows):
    def copy(k, slot):
        frame = k // per_frame
        rest = k % per_frame
        row = frame * band_rows + rest // across * SIDE
        return pltpu.make_async_copy(
            fmap.at[pl.ds(row, SIDE), rest % across],
            send.at[slot // SLOTS, pl.ds(slot % SLOTS * SIDE, SIDE)],
            sems.at[k],
        )

    return copy


def first_body(peers, blocks, tiles_of, per_frame, across, band_rows):
    last = LEVELS - 1

    def kernel(owner, tile, fmap, send, slots, count, labels, notes, sems, note_sem):
        copy = tile_copy(fmap, send, sems, per_frame, across, band_rows)

        def clear(i, carry):
            count[i] = 0
            return carry

        lax.fori_loop(0, LEVELS * peers, clear, 0, unroll=32)

        def blank(i, carry):
            labels[i] = 0
            return carry

        lax.fori_loop(0, LEVELS * SLOTS * peers, blank, 0, unroll=32)

        def place(k, carry):
            for level in reversed(range(LEVELS)):
                own = owner[level, 0, k]
                seen = count[level * peers + own]
                count[level * peers + own] = seen + 1
                slot = own * SLOTS + seen
                slots[level * blocks + k] = slot
                labels[level * SLOTS * peers + slot] = k // per_frame * tiles_of[level] + lax.rem(
                    tile[level, k], tiles_of[level]
                )
                if level == last:
                    copy(k, slot).start()
            return carry

        lax.fori_loop(0, blocks, place, 0, unroll=4)

        lane = lax.broadcasted_iota(jnp.int32, notes.shape[1:], 1)

        def note(peer, carry):
            values = jnp.zeros(notes.shape[1:], jnp.int32)
            for level in range(LEVELS):
                for seen in range(SLOTS):
                    label = labels[(level * peers + peer) * SLOTS + seen]
                    values = jnp.where(lane == level * SLOTS + seen, label, values)
            notes[peer] = values.astype(jnp.float32).astype(jnp.bfloat16)
            return carry

        lax.fori_loop(0, peers, note, 0, unroll=16)
        noted = pltpu.make_async_copy(notes, send.at[:, SLOTS * SIDE, :, pl.ds(0, 128)], note_sem)
        noted.start()

        def finish(k, carry):
            copy(k, slots[last * blocks + k]).wait()
            return carry

        lax.fori_loop(0, blocks, finish, 0, unroll=8)
        noted.wait()

    return kernel


def second_body(blocks, per_frame, across, band_rows):
    def kernel(slots, fmap, send, sems):
        copy = tile_copy(fmap, send, sems, per_frame, across, band_rows)

        def place(k, carry):
            copy(k, slots[k]).start()
            return carry

        def finish(k, carry):
            copy(k, slots[k]).wait()
            return carry

        lax.fori_loop(0, blocks, place, 0, unroll=4)
        lax.fori_loop(0, blocks, finish, 0, unroll=8)

    return kernel


def serve_body(level, rows, across, tiles, frames, peers):
    def kernel(notes, queries, strips, reply, flat, lines, labels, sem):
        step = pl.program_id(0)
        lane = lax.broadcasted_iota(jnp.int32, (1, LANES), 1)
        first = lane < QUERIES
        i_part = lane % QUERIES // SIDE
        j_part = lane % SIDE
        row_id = lax.broadcasted_iota(jnp.int32, (REPLY_ROWS, LANES), 0)

        @pl.when(step == 0)
        def _():
            flat[...] = jnp.zeros_like(flat)

            def line(peer, carry):
                values = notes[peer].astype(jnp.float32).astype(jnp.int32)
                lines[pl.ds(peer, 1), :] = values[:1, : lines.shape[1]]
                return carry

            lax.fori_loop(0, peers, line, 0, unroll=8)
            taken = pltpu.make_async_copy(lines, labels, sem)
            taken.start()
            taken.wait()

        def start_of(label):
            tile = label % tiles
            column = tile % across
            return (column * frames + label // tiles) * rows + tile // across * SIDE

        def one(peer, bench):
            query = queries[peer]
            tables = []
            for slot in range(SLOTS):
                label = labels[step * PEERS_A_STEP + peer, level * SLOTS + slot]
                cells = strips[pl.ds(start_of(label), SPAN)]
                tables.append(
                    lax.dot_general(
                        cells.reshape(SPAN * SPAN, -1),
                        query,
                        (((1,), (1,)), ((), ())),
                        preferred_element_type=jnp.float32,
                    )
                )
            table = jnp.where(first, tables[0], tables[1])
            table = table.reshape(SPAN, SPAN, LANES)
            for bit in (4, 2, 1):
                left = table.shape[0] - bit
                table = jnp.where(i_part & bit != 0, table[bit:], table[:left])
            table = table.reshape(WIN * SPAN, LANES)
            for bit in (4, 2, 1):
                table = jnp.where(
                    j_part & bit != 0, pltpu.roll(table, WIN * SPAN - bit, 0), table
                )
            for a in range(WIN):
                flat[bench, a * WIN : (a + 1) * WIN, :] = table[a * SPAN : a * SPAN + WIN]
            values = flat[bench]
            top = jnp.max(jnp.abs(values), axis=0, keepdims=True)
            power = jnp.ceil(jnp.log2(jnp.maximum(top, 1e-30)))
            coded = jnp.round(values * (jnp.exp2(-power) * FULL))
            coded = jnp.clip(coded, -FULL, FULL)
            coded = jnp.where(row_id == WINDOW, power, coded)
            reply[peer] = coded.astype(jnp.int32).astype(jnp.int16)

        def turn(i, carry):
            for bench in range(BENCHES):
                one(i * BENCHES + bench, bench)
            return carry

        lax.fori_loop(0, PEERS_A_STEP // BENCHES, turn, 0)

    return kernel


def finish_body(blocks, groups, scale):
    def kernel(slots, reply0, reply1, out):
        step = pl.program_id(0)
        low = lax.broadcasted_iota(jnp.int32, (1, LANES), 1) < QUERIES
        for level, reply in enumerate((reply0, reply1)):
            for group in range(groups):
                k = level * blocks + (step * groups + group) * 2
                slot = [slots[k + side] for side in range(2)]
                block = [reply[at // SLOTS].astype(jnp.int32) for at in slot]
                straight = jnp.where(low, block[0], block[1])
                turned = pltpu.roll(jnp.where(low, block[1], block[0]), QUERIES, 1)
                kept = [slot[side] % SLOTS == side for side in range(2)]
                left = jnp.where(kept[0], straight, turned)
                right = jnp.where(kept[1], straight, turned)
                both = jnp.where(low, left, right).astype(jnp.float32)
                factor = jnp.exp2(both[WINDOW : WINDOW + 1]) * (scale / FULL)
                out[:, level, group * LANES : (group + 1) * LANES] = both[:WINDOW] * factor

    return kernel


def steps(fmap1, fmap2, target_owner, target_tile):
    frames, band_rows, band_cols, channels = fmap1.shape
    peers = lax.axis_size("rows") * lax.axis_size("cols")
    across = band_cols // SIDE
    per_frame = band_rows // SIDE * across
    blocks = frames * per_frame
    across_of = [(band_cols >> l) // SIDE for l in range(LEVELS)]
    tiles_of = [((band_rows >> l) // SIDE) * across_of[l] for l in range(LEVELS)]

    smem = pl.BlockSpec(memory_space=pltpu.SMEM)
    vmem = pl.BlockSpec(memory_space=pltpu.VMEM)
    hbm = pl.BlockSpec(memory_space=pl.ANY)
    tiles = fmap1.reshape(frames * band_rows, across, SIDE, channels)

    def send_shape(parts):
        return jax.ShapeDtypeStruct((peers, parts, SIDE, channels), jnp.bfloat16)

    send1, slots = pl.pallas_call(
        first_body(peers, blocks, tiles_of, per_frame, across, band_rows),
        in_specs=[smem, smem, vmem],
        out_specs=[hbm, smem],
        out_shape=[
            send_shape(SLOTS * SIDE + 1),
            jax.ShapeDtypeStruct((LEVELS * blocks,), jnp.int32),
        ],
        scratch_shapes=[
            pltpu.SMEM((LEVELS * peers,), jnp.int32),
            pltpu.SMEM((LEVELS * SLOTS * peers,), jnp.int32),
            pltpu.VMEM((peers, SIDE, 128), jnp.bfloat16),
            pltpu.SemaphoreType.DMA((blocks,)),
            pltpu.SemaphoreType.DMA,
        ],
        name="build1",
    )(target_owner.transpose(0, 2, 1), target_tile, tiles)
    send0 = pl.pallas_call(
        second_body(blocks, per_frame, across, band_rows),
        in_specs=[smem, vmem],
        out_specs=hbm,
        out_shape=send_shape(SLOTS * SIDE),
        scratch_shapes=[pltpu.SemaphoreType.DMA((blocks,))],
        name="build0",
    )(slots, tiles)

    def exchange(value):
        return lax.all_to_all(value, AXES, split_axis=0, concat_axis=0, tiled=True)

    arrived = [exchange(send.reshape(peers, -1, channels)) for send in (send0, send1)]

    low, high = neighbours(fmap2, "rows", 1, SIDE)
    edges = [
        jnp.concatenate([lax.slice_in_dim(part, *span, axis=2) for part in (low, fmap2, high)], axis=1)
        for span in ((0, SIDE), (band_cols - SIDE, band_cols))
    ]
    west, east = swapped(edges[1], edges[0], "cols")
    tall = jnp.concatenate([low, fmap2, high], axis=1)
    wide = jnp.concatenate([west, tall, east], axis=2)
    maps = [wide[:, RADIUS:-RADIUS, RADIUS:-RADIUS], pool_level(wide)]

    replies = []
    for level in range(LEVELS):
        strips = window_strips(maps[level])
        served = pl.pallas_call(
            serve_body(level, maps[level].shape[1], across_of[level], tiles_of[level], frames, peers),
            grid=(peers // PEERS_A_STEP,),
            in_specs=[
                pl.BlockSpec((peers, SIDE, channels), lambda s: (0, LANES // SIDE, 0)),
                pl.BlockSpec((PEERS_A_STEP, LANES, channels), lambda s: (s, 0, 0)),
                pl.BlockSpec(strips.shape, lambda s: (0, 0, 0)),
            ],
            out_specs=pl.BlockSpec((PEERS_A_STEP, REPLY_ROWS, LANES), lambda s: (s, 0, 0)),
            scratch_shapes=[
                pltpu.VMEM((BENCHES, REPLY_ROWS, LANES), jnp.float32),
                pltpu.VMEM((peers, 128), jnp.int32),
                pltpu.SMEM((peers, 128), jnp.int32),
                pltpu.SemaphoreType.DMA,
            ],
            out_shape=jax.ShapeDtypeStruct((peers, REPLY_ROWS, LANES), jnp.int16),
        )(arrived[1], arrived[level], strips)
        replies.append(exchange(served))

    groups = 8
    width = groups * LANES
    whole = pl.BlockSpec((peers, REPLY_ROWS, LANES), lambda s, _: (0, 0, 0))
    out = pl.pallas_call(
        finish_body(blocks, groups, channels ** (-0.5)),
        grid_spec=pltpu.PrefetchScalarGridSpec(
            num_scalar_prefetch=1,
            grid=(blocks * QUERIES // width,),
            in_specs=[whole, whole],
            out_specs=pl.BlockSpec((WINDOW, LEVELS, width), lambda s, _: (0, 0, s)),
        ),
        out_shape=jax.ShapeDtypeStruct((WINDOW, LEVELS, blocks * QUERIES), jnp.float32),
        compiler_params=pltpu.CompilerParams(vmem_limit_bytes=FINISH_VMEM),
        name="finish",
    )(slots, *replies)
    return out.transpose(1, 0, 2)


def solution(mesh):
    in_specs = (
        P(None, "rows", "cols", None),
        P(None, "rows", "cols", None),
        P(None, AXES, None),
        P(None, AXES),
    )
    out_specs = P(None, None, AXES)
    return jax.shard_map(steps, mesh=mesh, in_specs=in_specs, out_specs=out_specs, check_vma=False)
```
